128 devices in a mesh: grp: 4 (over z), seq: 32 (over x, y, core).
Axes of the slice: x: 4, y: 4, z: 4, core: 2. Of those that a mesh axis runs over, the one named last changes fastest.
Arguments:
- stream: bfloat16 [16384, 2048], P(('grp', 'seq')), may hold values from -64 to 64
- cotangent: bfloat16 [16384, 2048], P(('grp', 'seq')), may hold values from -6 to 6
- norm_gain: float32 [2048], replicated, may hold values from 0.5 to 1.5
- queries: bfloat16 [16384, 2048], P(('grp', 'seq')), may hold values from -6 to 6
- key_vectors: bfloat16 [16384, 2048], P(('grp', 'seq')), may hold values from -6 to 6
- value_vectors: bfloat16 [16384, 2048], P(('grp', 'seq')), may hold values from -6 to 6
- expert_index: int32 [128, 256], replicated, may hold values from 0 to 16383, as said below
- router_gates: float32 [128, 256], P(('grp', 'seq')), may hold values from 0.05 to 1
- gate_proj: bfloat16 [128, 2048, 768], P(('grp', 'seq')), may hold values from -0.125 to 0.125
- up_proj: bfloat16 [128, 2048, 768], P(('grp', 'seq')), may hold values from -0.125 to 0.125
- down_proj: bfloat16 [128, 768, 2048], P(('grp', 'seq')), may hold values from -0.21875 to 0.21875
Outputs:
- grad_stream: bfloat16 [16384, 2048], P(('grp', 'seq'))
- grad_queries: bfloat16 [16384, 2048], P(('grp', 'seq'))
- grad_keys: bfloat16 [16384, 2048], P(('grp', 'seq'))
- grad_values: bfloat16 [16384, 2048], P(('grp', 'seq'))
- grad_gate: bfloat16 [128, 2048, 768], P(('grp', 'seq'))
- grad_up: bfloat16 [128, 2048, 768], P(('grp', 'seq'))
- grad_down: bfloat16 [128, 768, 2048], P(('grp', 'seq'))
- grad_router: float32 [128, 256], P(('grp', 'seq'))
- grad_norm_gain: float32 [2048], replicated
The draws below stay inside these ranges and needn't reach their ends.
Inputs may be any that keep to these rules, and one draw needn't show every extreme that they name: `expert_index`: row e holds 256 different token numbers. Of the 128 tokens numbered d * 128 to (d + 1) * 128 - 1, one expert chooses at most 4, and in every row some d has exactly 4 chosen.
All inputs are finite; a program needn't handle non-finite values.
Results may differ from the reference program's by a relative error of at most 0.024.
Values may be sent and summed in bfloat16 or wider, within the bound.
A program may use at most 192 MiB of HBM per device.

```python
import math
import jax
import jax.numpy as jnp
from jax import lax

D = 2048
FF = 768
HEADS = 16
HEAD = 128
CAP = 256
BLOCK = 128
T_DEV = 128
EXPERTS = 128
TOKENS = 16384
N_GRP = 4
N_SEQ = 32


def draw_stream(key, part):
    first, second = jax.random.split(key, 2)
    row_scale = jnp.exp(jax.random.uniform(second, (TOKENS, 1), jnp.float32) * math.log(10.0))
    base = jax.random.normal(first, (TOKENS, D), jnp.float32)
    return jnp.clip(base * row_scale, -64.0, 64.0).astype(jnp.bfloat16)


def choose_rows(expert_key):
    block_count = TOKENS // T_DEV
    half = block_count // 2
    base = CAP // block_count
    first, second, third, fourth = jax.random.split(expert_key, 4)
    shuffled = jax.random.permutation(first, block_count)
    delta = jax.random.randint(second, (half,), -base, base + 1)
    delta = delta.at[0].set(base)
    counts = jnp.full((block_count,), base, jnp.int32)
    counts = counts.at[shuffled[:half]].add(delta).at[shuffled[half:]].add(-delta)
    scores = jax.random.randint(third, (block_count, T_DEV), 0, 1 << 20) * T_DEV + jnp.arange(T_DEV)[None, :]
    ordering = jnp.argsort(scores, axis=1)
    ranking = jnp.argsort(ordering, axis=1)
    chosen = (ranking < counts[:, None]).reshape(-1)
    sort_key = jnp.where(chosen, 0, 1) * TOKENS + jnp.arange(TOKENS)
    picked = jnp.argsort(sort_key)[:CAP]
    mixing = jax.random.permutation(fourth, CAP)
    return picked[mixing].astype(jnp.int32)


def draw_expert_index(key, part):
    expert_keys = jax.random.split(jax.random.fold_in(key, 17), EXPERTS)
    return jax.vmap(choose_rows)(expert_keys).astype(jnp.int32)


def level_of(stream_key, shape, shards, least, top_value):
    factor_of = 1.0
    for dim, blocks in shards:
        steps = jax.random.uniform(jax.random.fold_in(jax.random.fold_in(stream_key, 6), dim), (blocks,), jnp.float32, least / len(shards), top_value / len(shards))
        factor_of = factor_of * jnp.repeat(jnp.exp(steps), shape[dim] // blocks).reshape((-1,) + (1,) * (len(shape) - 1 - dim))
    return factor_of


def bell_draw(rng, extent, scale, limit, pieces=(), held_as=jnp.bfloat16):
    level = level_of(rng, extent, pieces, -0.22, 0.18) if pieces else 1.0
    array = jax.random.normal(rng, extent, jnp.float32) * scale * level
    return jnp.minimum(jnp.maximum(array, -limit), limit).astype(held_as)


def setup_inputs(seed: int = 0) -> dict:
    key_of = jax.random.split(jax.random.key(seed), 12)
    return {
        "stream": draw_stream(jax.random.fold_in(key_of[11], 71), 0),
        "cotangent": bell_draw(key_of[1], (TOKENS, D), 1.0, 6.0, ((0, 128),)),
        "norm_gain": jnp.clip(1.0 + 0.1 * jax.random.normal(key_of[2], (D,), jnp.float32), 0.5, 1.5),
        "queries": bell_draw(key_of[3], (TOKENS, D), 1.0, 6.0, ((0, 128),)),
        "key_vectors": bell_draw(key_of[4], (TOKENS, D), 1.0, 6.0, ((0, 128),)),
        "value_vectors": bell_draw(key_of[5], (TOKENS, D), 1.0, 6.0, ((0, 128),)),
        "expert_index": draw_expert_index(jax.random.fold_in(key_of[11], 71), 0),
        "router_gates": jnp.clip(0.05 + 0.95 * jax.random.uniform(key_of[7], (EXPERTS, CAP), jnp.float32) ** level_of(key_of[7], (EXPERTS, CAP), ((0, 128),), -0.2, 0.2), 0.05, 1.0),
        "gate_proj": bell_draw(key_of[8], (EXPERTS, D, FF), D ** -0.5, 0.125, ((0, 128),)),
        "up_proj": bell_draw(key_of[9], (EXPERTS, D, FF), D ** -0.5, 0.125, ((0, 128),)),
        "down_proj": bell_draw(key_of[10], (EXPERTS, FF, D), FF ** -0.5, 0.21875, ((0, 128),)),
    }


EPS = 1e-06

def expert_back(rows, dy_rows, gates, w_gate, w_up, w_down):
    gate_pre = jnp.dot(rows, w_gate, preferred_element_type=jnp.float32)
    up_pre = jnp.dot(rows, w_up, preferred_element_type=jnp.float32)
    sigmoid_gate = jax.nn.sigmoid(gate_pre)
    silu_gate = gate_pre * sigmoid_gate
    hidden = (silu_gate * up_pre).astype(jnp.bfloat16)
    expert_out = jnp.dot(hidden, w_down, preferred_element_type=jnp.float32)
    grad_router = lax.optimization_barrier(jnp.sum(dy_rows.astype(jnp.float32) * expert_out, axis=1))
    grad_out = (gates[:, None] * dy_rows.astype(jnp.float32)).astype(jnp.bfloat16)
    grad_down = jnp.dot(hidden.T, grad_out, preferred_element_type=jnp.float32).astype(jnp.bfloat16)
    grad_hidden = jnp.dot(grad_out, w_down.T, preferred_element_type=jnp.float32)
    slope = sigmoid_gate * (1.0 + gate_pre * (1.0 - sigmoid_gate))
    grad_gate_pre = (grad_hidden * up_pre * slope).astype(jnp.bfloat16)
    grad_up_pre = (grad_hidden * silu_gate).astype(jnp.bfloat16)
    grad_gate = jnp.dot(rows.T, grad_gate_pre, preferred_element_type=jnp.float32).astype(jnp.bfloat16)
    grad_up = jnp.dot(rows.T, grad_up_pre, preferred_element_type=jnp.float32).astype(jnp.bfloat16)
    grad_rows = (jnp.dot(grad_gate_pre, w_gate.T, preferred_element_type=jnp.float32) + jnp.dot(grad_up_pre, w_up.T, preferred_element_type=jnp.float32)).astype(jnp.bfloat16)
    return (grad_rows, grad_gate, grad_up, grad_down, grad_router)

def rounded(values):
    return lax.optimization_barrier(values.astype(jnp.bfloat16)).astype(jnp.float32)

def reference(stream, cotangent, norm_gain, queries, key_vectors, value_vectors, expert_index, router_gates, gate_proj, up_proj, down_proj):
    wide_stream = stream.astype(jnp.float32)
    inverse_rms = lax.rsqrt(lax.optimization_barrier(jnp.mean(wide_stream * wide_stream, axis=1, keepdims=True)) + EPS)
    normed = wide_stream * inverse_rms
    inputs = (normed * norm_gain[None, :]).astype(jnp.bfloat16)

    def expert_step(accum, expert_item):
        chosen, gates, w_gate, w_up, w_down = expert_item
        grad_rows, grad_gate, grad_up, grad_down, grad_router = expert_back(inputs[chosen], cotangent[chosen], gates, w_gate, w_up, w_down)
        accum = accum.at[chosen].add(grad_rows.astype(jnp.float32))
        return (accum, (grad_gate, grad_up, grad_down, grad_router))
    start = jnp.zeros((TOKENS, D), jnp.float32)
    grad_inputs, (grad_gate, grad_up, grad_down, grad_router) = lax.scan(expert_step, start, (expert_index, router_gates, gate_proj, up_proj, down_proj))
    grad_norm_gain = lax.optimization_barrier(jnp.sum(grad_inputs * normed, axis=0))
    grad_normed = grad_inputs * norm_gain[None, :]
    grad_wide = cotangent.astype(jnp.float32) + inverse_rms * (grad_normed - normed * lax.optimization_barrier(jnp.mean(grad_normed * normed, axis=1, keepdims=True)))
    grad_stream = grad_wide.astype(jnp.bfloat16)
    blocks = T_DEV * N_SEQ // BLOCK
    scale = 1.0 / jnp.sqrt(jnp.float32(HEAD * T_DEV * N_SEQ))

    def shaped(values):
        return values.astype(jnp.float32).reshape(N_GRP, blocks, BLOCK, HEADS, HEAD)
    qq, kk, vv, gg = (shaped(queries), shaped(key_vectors), shaped(value_vectors), shaped(grad_stream))
    lower = jnp.arange(BLOCK)[:, None] >= jnp.arange(BLOCK)[None, :]
    high = lax.Precision.HIGHEST
    mix_a = rounded(jnp.where(lower, jnp.einsum('gntha,gnsha->gnhts', gg, vv, precision=high), 0.0))
    mix_b = rounded(jnp.where(lower, jnp.einsum('gntha,gnsha->gnhts', qq, kk, precision=high), 0.0))
    inc_state = jnp.einsum('gnsha,gnshb->gnhab', kk, vv, precision=high)
    inc_grad = jnp.einsum('gntha,gnthb->gnhab', qq, gg, precision=high)
    prior_state = jnp.cumsum(inc_state, axis=1) - inc_state
    later_state = jnp.cumsum(inc_grad[:, ::-1], axis=1)[:, ::-1] - inc_grad
    grad_q = scale * (jnp.einsum('gnhts,gnsha->gntha', mix_a, kk, precision=high) + jnp.einsum('gnthb,gnhab->gntha', gg, prior_state, precision=high))
    grad_k = scale * (jnp.einsum('gnhts,gntha->gnsha', mix_a, qq, precision=high) + jnp.einsum('gnshb,gnhab->gnsha', vv, later_state, precision=high))
    grad_v = scale * (jnp.einsum('gnhts,gnthb->gnshb', mix_b, gg, precision=high) + jnp.einsum('gnsha,gnhab->gnshb', kk, later_state, precision=high))
    grad_queries = grad_q.reshape(TOKENS, D).astype(jnp.bfloat16)
    grad_keys = grad_k.reshape(TOKENS, D).astype(jnp.bfloat16)
    grad_values = grad_v.reshape(TOKENS, D).astype(jnp.bfloat16)
    return (grad_stream, grad_queries, grad_keys, grad_values, grad_gate, grad_up, grad_down, grad_router, grad_norm_gain)
```

```python
import functools
import math

import jax
import jax.numpy as jnp
from jax import lax
from jax.experimental import pallas as pl
from jax.experimental.pallas import tpu as pltpu
from jax.sharding import PartitionSpec as P

D = 2048
FF = 768
HEADS = 16
HEAD = 128
CAP = 256
TOK = 128
DEV = 128
PLANE = 32
SLOTS = 4
EPS = 1e-06
MULT = 37
MULT_INV = 45
PLANE_MULT = 13
MESH = pl.DeviceIdType.MESH
BF = jnp.bfloat16
F32 = jnp.float32


def dot(a, b):
    return lax.dot_general(a, b, (((1,), (0,)), ((), ())), preferred_element_type=F32)


def dot_nt(a, b):
    return lax.dot_general(a, b, (((1,), (1,)), ((), ())), preferred_element_type=F32)


def dot_tn(a, b):
    return lax.dot_general(a, b, (((0,), (0,)), ((), ())), preferred_element_type=F32)


def rem(a, n):
    return lax.rem(a, jnp.int32(n))


def div(a, n):
    return lax.div(a, jnp.int32(n))


def offsets(i):
    k = rem(i * MULT, DEV)
    return div(k, 32), rem(div(k, 8), 4), rem(div(k, 2), 4), rem(k, 2)


def index_of(z, x, y, c):
    return rem(z, 4), rem(x, 4) * 8 + rem(y, 4) * 2 + rem(c, 2)


def mega(
    stream_h, cot_h, gain_h, code_h, tcol_h, trow_h, gates_h, wg_h, wu_h, wd_h, q_h, k_h, v_h,
    rows_o, gout_o, hid_o, dgp_o, dup_o, router_o, g_o, prior_o, later_o, gain_o,
    stream, cot, gain, code, tcol, trow, gates, wg, wu, wd, qv, kv, vv,
    normed, xin, p8, send, recv, acc, rows, gout, hid, dgp, dup, stacked, rsend, rrecv,
    gin, g, skv, sqg, kv1, kvs, kv2, qg1, qgs, qg2, gpart, gland, router,
    lsem, osem, fsem, frsem, bsem, brsem, asem, arsem, gsem, grsem, zsem,
):
    z = lax.axis_index("grp")
    s = lax.axis_index("seq")
    x, y, c = div(s, 8), rem(div(s, 2), 4), rem(s, 2)

    def dev(z2, s2):
        return {"grp": z2, "seq": s2}

    def out_to(i):
        dz, dx, dy, dc = offsets(i)
        return dev(*index_of(z + dz, x + dx, y + dy, c + dc))

    def back_to(i):
        dz, dx, dy, dc = offsets(i)
        return dev(*index_of(z + 4 - dz, x + 4 - dx, y + 4 - dy, c + dc))

    def plane_to(j):
        k = rem(j * PLANE_MULT, PLANE)
        return index_of(z, x + div(k, 8), y + rem(div(k, 2), 4), c + rem(k, 2))[1]

    bar = pltpu.get_barrier_semaphore()

    def greet(j, carry):
        pl.semaphore_signal(bar, inc=1, device_id=dev(z, plane_to(j)), device_id_type=MESH)
        return carry

    lax.fori_loop(1, PLANE, greet, 0)
    for d in (1, 2, 3):
        pl.semaphore_signal(bar, inc=1, device_id=dev(rem(z + d, 4), s), device_id_type=MESH)

    loads = [
        (stream_h, stream), (cot_h, cot), (gain_h, gain), (code_h, code), (tcol_h, tcol), (trow_h, trow),
        (gates_h, gates), (q_h, qv), (k_h, kv), (v_h, vv), (wg_h, wg), (wu_h, wu), (wd_h, wd),
    ]
    load = [pltpu.make_async_copy(a, b, lsem.at[n]) for n, (a, b) in enumerate(loads)]
    for cp in load:
        cp.start()

    for n in (0, 1, 2, 3):
        load[n].wait()
    wide = stream[...].astype(F32)
    inv = lax.rsqrt(jnp.mean(wide * wide, axis=1, keepdims=True) + EPS)
    nrm = wide * inv
    normed[...] = nrm
    xin[0:TOK, :] = (nrm * gain[...]).astype(BF)
    xin[TOK:, :] = cot[...]

    def build(gi, carry):
        r = lax.broadcasted_iota(jnp.int32, (256, 128), 0) + gi * 256
        lane = lax.broadcasted_iota(jnp.int32, (256, 128), 1)
        k = ((r >> 3) * MULT) & (DEV - 1)
        e = ((z + (k >> 5)) & 3) * 32 + ((x + (k >> 3)) & 3) * 8 + ((y + (k >> 1)) & 3) * 2 + ((c + k) & 1)
        pick = jnp.where(e == lane, 1.0, 0.0).astype(BF)
        rep = dot(pick, code[...])
        want = ((r & 3) + 1).astype(F32)
        hit = jnp.where(rep == want, 1.0, 0.0)
        kind = (r >> 2) & 1
        row0 = pl.multiple_of(gi * 256, 256)
        p8[pl.ds(row0, 256), 0:128] = jnp.where(kind == 0, hit, 0.0).astype(BF)
        p8[pl.ds(row0, 256), 128:256] = jnp.where(kind == 1, hit, 0.0).astype(BF)
        return carry

    lax.fori_loop(0, 4, build, 0)

    def fill(gi, carry):
        row0 = pl.multiple_of(gi * 256, 256)
        sel = p8[pl.ds(row0, 256), :]
        lo = dot(sel, xin[:, 0:1024]).reshape(32, 8, 1024)
        hi = dot(sel, xin[:, 1024:2048]).reshape(32, 8, 1024)
        send[pl.ds(gi * 32, 32)] = jnp.concatenate([lo, hi], axis=1).astype(BF)
        return carry

    lax.fori_loop(0, 4, fill, 0)

    pl.semaphore_wait(bar, PLANE - 1 + 3)
    for d in (1, 2, 3):
        pl.semaphore_signal(zsem, inc=1, device_id=dev(rem(z + d, 4), s), device_id_type=MESH)
    pl.semaphore_wait(zsem, 3)

    def push(i, carry):
        pltpu.make_async_remote_copy(
            send.at[i], recv.at[i], fsem, frsem.at[div(i, 32)], device_id=out_to(i), device_id_type=MESH
        ).start()
        return carry

    lax.fori_loop(1, DEV, push, 0)
    recv[0] = send[0]

    load[7].wait()
    load[8].wait()
    load[9].wait()
    for h in range(HEADS):
        kh = kv[:, h * HEAD:(h + 1) * HEAD]
        vh = vv[:, h * HEAD:(h + 1) * HEAD]
        skv[2 * h:2 * h + 2] = dot_tn(kh, vh).reshape(2, 64, HEAD).astype(BF)

    load[4].wait()
    load[5].wait()
    load[6].wait()

    acc[...] = jnp.zeros_like(acc)
    for gi in range(4):
        first = 1 if gi == 0 else 0
        span = recv.at[pl.ds(gi * 32 + first, 32 - first)]
        pltpu.make_async_copy(span, span, frsem.at[gi]).wait()
        lane = lax.broadcasted_iota(jnp.int32, (512, 256), 1) + gi * 256
        put = jnp.where(lane == tcol[:, 0:1], 1.0, 0.0).astype(BF)
        for half in range(2):
            f = recv[pl.ds(gi * 32, 32)].astype(F32).reshape(32, 2, 8, 1024)[:, half]
            f = f.reshape(256, 1024).astype(BF)
            acc[:, half * 1024:(half + 1) * 1024] += dot(put, f)

    def scatter(src, dst, sem, rsem):
        def one(j, carry):
            to = plane_to(j)
            pltpu.make_async_remote_copy(
                src.at[to], dst.at[s], sem, rsem, device_id=dev(z, to), device_id_type=MESH
            ).start()
            return carry

        lax.fori_loop(1, PLANE, one, 0)
        dst[s] = src[s]

    def arrived(dst, rsem):
        span = dst.at[pl.ds(0, PLANE - 1)]
        pltpu.make_async_copy(span, span, rsem).wait()

    scatter(skv, kv1, asem.at[0], arsem.at[0])

    rows[...] = acc[0:CAP, :].astype(BF)
    dyf = acc[CAP:, :]
    gout[...] = (gates[:, 0:1] * dyf).astype(BF)
    for n in (10, 11, 12):
        load[n].wait()

    def front(n, carry):
        c0 = pl.multiple_of(n * 256, 256)
        gp = dot(rows[...], wg[:, pl.ds(c0, 256)])
        up = dot(rows[...], wu[:, pl.ds(c0, 256)])
        gh = dot_nt(gout[...], wd[pl.ds(c0, 256), :])
        sg = jax.nn.sigmoid(gp)
        silu = gp * sg
        hid[:, pl.ds(c0, 256)] = (silu * up).astype(BF)
        dgp[:, pl.ds(c0, 256)] = (gh * up * (sg * (1.0 + gp * (1.0 - sg)))).astype(BF)
        dup[:, pl.ds(c0, 256)] = (gh * silu).astype(BF)
        return carry

    lax.fori_loop(0, 3, front, 0)

    def back(n, carry):
        r0 = pl.multiple_of(n * 256, 256)
        gr = dot_nt(dgp[...], wg[pl.ds(r0, 256), :]) + dot_nt(dup[...], wu[pl.ds(r0, 256), :])
        h0 = pl.multiple_of(div(n, 4) * 256, 256)
        c0 = pl.multiple_of(rem(n, 4) * 256, 256)
        stacked[pl.ds(h0, 256), pl.ds(c0, 256)] = gr.astype(BF)
        return carry

    lax.fori_loop(0, 8, back, 0)

    def refill(gi, carry):
        r = lax.broadcasted_iota(jnp.int32, (256, 512), 0) + gi * 256
        put = jnp.where(r == trow[...], 1.0, 0.0).astype(BF)
        o = dot(put, stacked[...]).reshape(32, 8, 1024)
        o = jnp.concatenate([o[:, :, 0:512], o[:, :, 512:1024]], axis=1)
        rsend[pl.ds(gi * 32, 32)] = o.astype(BF)
        return carry

    def ret(i, carry):
        pltpu.make_async_remote_copy(
            rsend.at[i], rrecv.at[i], bsem, brsem.at[div(i, 32)], device_id=back_to(i), device_id_type=MESH
        ).start()
        return carry

    lax.fori_loop(0, 2, refill, 0)
    lax.fori_loop(1, 32, ret, 0)
    lax.fori_loop(2, 3, refill, 0)
    lax.fori_loop(32, 64, ret, 0)
    lax.fori_loop(3, 4, refill, 0)
    lax.fori_loop(64, 128, ret, 0)
    rrecv[0] = rsend[0]

    outs = [(rows, rows_o), (gout, gout_o), (hid, hid_o), (dgp, dgp_o), (dup, dup_o)]
    store = [pltpu.make_async_copy(a, b, osem.at[n]) for n, (a, b) in enumerate(outs)]
    for cp in store:
        cp.start()

    def route(n, total):
        c0 = pl.multiple_of(n * 256, 256)
        eo = dot(hid[...], wd[:, pl.ds(c0, 256)])
        return total + jnp.sum(acc[CAP:, pl.ds(c0, 256)] * eo, axis=1, keepdims=True)

    router[...] = jnp.broadcast_to(lax.fori_loop(0, 8, route, jnp.zeros((CAP, 1), F32)), router.shape)

    arrived(kv1, arsem.at[0])

    def prefix(r, total):
        kvs[r] = total.astype(BF)
        return total + kv1[r].astype(F32)

    lax.fori_loop(0, PLANE, prefix, jnp.zeros((64, HEAD), F32))

    for gi in range(4):
        first = 1 if gi == 0 else 0
        span = rrecv.at[pl.ds(gi * 32 + first, 32 - first)]
        pltpu.make_async_copy(span, span, brsem.at[gi]).wait()
        for half in range(2):
            f = rrecv[pl.ds(gi * 32, 32)].astype(F32).reshape(32, 2, 8, 512)[:, half]
            f = f.reshape(256, 512).astype(BF)
            part = dot_tn(p8[gi * 256:(gi + 1) * 256, :], f)
            for hh in range(2):
                c0 = hh * 1024 + half * 512
                piece = part[hh * TOK:(hh + 1) * TOK, :]
                if gi == 0:
                    gin[:, c0:c0 + 512] = piece
                else:
                    gin[:, c0:c0 + 512] += piece

    scatter(kvs, kv2, asem.at[1], arsem.at[1])

    gi_ = gin[...]
    nrm = normed[...]

    def spread(stage):
        if stage == 0:
            to = [dev(z, s + 1 - 2 * c)]
        elif stage == 1:
            to = [dev(z, x * 8 + rem(y + d, 4) * 2 + c) for d in (1, 2, 3)]
        elif stage == 2:
            to = [dev(z, rem(x + d, 4) * 8 + y * 2 + c) for d in (1, 2, 3)]
        else:
            to = [dev(rem(z + d, 4), s) for d in (1, 2, 3)]
        cps = [
            pltpu.make_async_remote_copy(
                gpart.at[stage], gland.at[stage, d], gsem.at[stage, d], grsem.at[stage, d],
                device_id=t, device_id_type=MESH,
            )
            for d, t in enumerate(to)
        ]
        for cp in cps:
            cp.start()
        return cps

    def collect(stage, cps):
        for cp in cps:
            cp.wait()
        total = gpart[stage]
        for d in range(len(cps)):
            total = total + gland[stage, d]
        return total

    gpart[0] = jnp.sum(gi_ * nrm, axis=0, keepdims=True)
    cps0 = spread(0)

    gn = gi_ * gain[...]
    wide_g = cot[...].astype(F32) + inv * (gn - nrm * jnp.mean(gn * nrm, axis=1, keepdims=True))
    g[...] = wide_g.astype(BF)
    gcp = pltpu.make_async_copy(g, g_o, osem.at[5])
    gcp.start()
    for h in range(HEADS):
        qh = qv[:, h * HEAD:(h + 1) * HEAD]
        gh = g[:, h * HEAD:(h + 1) * HEAD]
        sqg[2 * h:2 * h + 2] = dot_tn(qh, gh).reshape(2, 64, HEAD).astype(BF)
    scatter(sqg, qg1, asem.at[2], arsem.at[2])
    gpart[1] = collect(0, cps0)
    cps1 = spread(1)
    arrived(qg1, arsem.at[2])

    def suffix(n, total):
        r = PLANE - 1 - n
        qgs[r] = total.astype(BF)
        return total + qg1[r].astype(F32)

    lax.fori_loop(0, PLANE, suffix, jnp.zeros((64, HEAD), F32))
    scatter(qgs, qg2, asem.at[3], arsem.at[3])
    gpart[2] = collect(1, cps1)
    cps2 = spread(2)
    arrived(kv2, arsem.at[1])
    pcp = pltpu.make_async_copy(kv2, prior_o, osem.at[6])
    pcp.start()
    gpart[3] = collect(2, cps2)
    cps3 = spread(3)
    arrived(qg2, arsem.at[3])
    lcp = pltpu.make_async_copy(qg2, later_o, osem.at[7])
    lcp.start()
    gpart[4] = collect(3, cps3)
    ncp = pltpu.make_async_copy(gpart.at[4], gain_o, osem.at[8])
    ncp.start()
    rcp = pltpu.make_async_copy(router, router_o, osem.at[9])
    rcp.start()

    span = send.at[pl.ds(1, DEV - 1)]
    pltpu.make_async_copy(span, span, fsem).wait()
    span = rsend.at[pl.ds(1, DEV - 1)]
    pltpu.make_async_copy(span, span, bsem).wait()
    for n, buf in enumerate((skv, kvs, sqg, qgs)):
        arrived(buf, asem.at[n])
    for cp in store + [gcp, pcp, lcp, ncp, rcp]:
        cp.wait()


def call_mega(operands):
    def vm(shape, dtype):
        return pltpu.VMEM(shape, dtype)

    state = (PLANE, 64, HEAD)
    results = [
        ((CAP, D), BF), ((CAP, D), BF), ((CAP, FF), BF), ((CAP, FF), BF), ((CAP, FF), BF), ((CAP, 128), F32),
        ((TOK, D), BF), (state, BF), (state, BF), ((1, D), F32),
    ]
    scratch = [
        vm((TOK, D), BF), vm((TOK, D), BF), vm((1, D), F32), vm((DEV, TOK), BF), vm((512, 128), jnp.int32),
        vm((1, 512), jnp.int32), vm((CAP, 128), F32), vm((D, FF), BF), vm((D, FF), BF), vm((FF, D), BF),
        vm((TOK, D), BF), vm((TOK, D), BF), vm((TOK, D), BF),
        vm((TOK, D), F32), vm((2 * TOK, D), BF), vm((1024, 256), BF), vm((DEV, 16, 1024), BF),
        vm((DEV, 16, 1024), BF), vm((512, D), F32), vm((CAP, D), BF), vm((CAP, D), BF),
        vm((CAP, FF), BF), vm((CAP, FF), BF), vm((CAP, FF), BF), vm((512, 1024), BF),
        vm((DEV, 16, 512), BF), vm((DEV, 16, 512), BF),
        vm((TOK, D), F32), vm((TOK, D), BF),
    ] + [vm(state, BF)] * 8 + [
        vm((5, 1, D), F32), vm((4, 3, 1, D), F32), vm((CAP, 128), F32),
    ]
    dma = pltpu.SemaphoreType.DMA
    sems = [
        dma((13,)), dma((10,)), dma, dma((4,)), dma, dma((4,)), dma((4,)), dma((4,)), dma((4, 3)), dma((4, 3)),
        pltpu.SemaphoreType.REGULAR,
    ]
    return pl.pallas_call(
        mega,
        out_shape=[jax.ShapeDtypeStruct(a, b) for a, b in results],
        in_specs=[pl.BlockSpec(memory_space=pl.ANY)] * 13,
        out_specs=[pl.BlockSpec(memory_space=pl.ANY)] * len(results),
        scratch_shapes=scratch + sems,
        compiler_params=pltpu.CompilerParams(
            collective_id=0, has_side_effects=True, vmem_limit_bytes=63 * 1024 * 1024
        ),
        name="mega",
    )(*operands)


def attend(scale, q_ref, k_ref, v_ref, g_ref, prior_ref, later_ref, gq_ref, gk_ref, gv_ref):
    q, k, v, g = q_ref[...], k_ref[...], v_ref[...], g_ref[...]
    prior = prior_ref[...].reshape(HEAD, HEAD)
    later = later_ref[...].reshape(HEAD, HEAD)
    row = lax.broadcasted_iota(jnp.int32, (TOK, TOK), 0)
    col = lax.broadcasted_iota(jnp.int32, (TOK, TOK), 1)
    mix_a = jnp.where(row >= col, dot_nt(g, v), 0.0).astype(BF)
    mix_b = jnp.where(row >= col, dot_nt(q, k), 0.0).astype(BF)
    gq_ref[...] = (scale * (dot(mix_a, k) + dot_nt(g, prior))).astype(BF)
    gk_ref[...] = (scale * (dot_tn(mix_a, q) + dot_nt(v, later))).astype(BF)
    gv_ref[...] = (scale * (dot_tn(mix_b, g) + dot(k, later))).astype(BF)


def call_attend(scale, q, k, v, g, prior, later):
    tok = pl.BlockSpec((TOK, HEAD), lambda h: (0, h))
    st = pl.BlockSpec((2, 64, HEAD), lambda h: (h, 0, 0))
    return pl.pallas_call(
        functools.partial(attend, scale),
        grid=(HEADS,),
        out_shape=[jax.ShapeDtypeStruct((TOK, D), BF)] * 3,
        in_specs=[tok] * 4 + [st] * 2,
        out_specs=[tok] * 3,
        name="attend",
    )(q, k, v, g, prior, later)


def body(stream, cotangent, norm_gain, queries, key_vectors, value_vectors, expert_index, router_gates,
         gate_proj, up_proj, down_proj):
    z = lax.axis_index("grp")
    s = lax.axis_index("seq")
    here = z * PLANE + s
    local = expert_index - here * TOK
    t = jnp.arange(TOK)
    same = jnp.sum((local[:, None, :] == t[None, :, None]).astype(jnp.int32), axis=2)
    under = jnp.sum(
        ((local[:, None, :] >= 0) & (local[:, None, :] < t[None, :, None])).astype(jnp.int32), axis=2
    )
    code = (same * (under + 1)).astype(BF)
    own = lax.dynamic_index_in_dim(expert_index, here, 0, keepdims=False)
    src = own // TOK
    slot = jnp.sum((src[None, :] == src[:, None]) & (own[None, :] < own[:, None]), axis=1).astype(jnp.int32)
    x, y, c = s // 8, (s // 2) % 4, s % 2
    dz = (z - src // 32) % 4
    dx = (x - (src // 8) % 4) % 4
    dy = (y - (src // 2) % 4) % 4
    dc = (c - src % 2) % 2
    at = ((dz * 32 + dx * 8 + dy * 2 + dc) * MULT_INV) % DEV
    target = at * 8 + slot
    target = jnp.concatenate([target, target + 4])
    tcol = jnp.broadcast_to(target[:, None], (512, 128))
    trow = target[None, :]
    gates = jnp.broadcast_to(router_gates[0][:, None], (CAP, 128))
    rows, gout, hid, dgp, dup, router, g, prior, later, gain = call_mega(
        (stream, cotangent, norm_gain[None, :], code, tcol, trow, gates, gate_proj[0], up_proj[0], down_proj[0],
         queries, key_vectors, value_vectors)
    )
    scale = 1.0 / math.sqrt(HEAD * TOK * PLANE)
    gq, gk, gv = call_attend(scale, queries, key_vectors, value_vectors, g, prior, later)
    grad_down = dot_tn(hid, gout).astype(BF)
    grad_gate = dot_tn(rows, dgp).astype(BF)
    grad_up = dot_tn(rows, dup).astype(BF)
    return (g, gq, gk, gv, grad_gate[None], grad_up[None], grad_down[None], router[:, 0][None], gain[0])


def solution(mesh):
    both = ("grp", "seq")
    r2, r3 = P(both, None), P(both, None, None)
    return jax.shard_map(
        body,
        mesh=mesh,
        in_specs=(r2, r2, P(), r2, r2, r2, P(), r2, r3, r3, r3),
        out_specs=(r2, r2, r2, r2, r3, r3, r3, r2, P()),
        check_vma=False,
    )
```

```python
import functools
import math

import jax
import jax.numpy as jnp
from jax import lax
from jax.experimental import pallas as pl
from jax.experimental.pallas import tpu as pltpu
from jax.sharding import PartitionSpec as P

D = 2048
FF = 768
HEADS = 16
HEAD = 128
CAP = 256
TOK = 128
DEV = 128
PLANE = 32
SLOTS = 4
EPS = 1e-06
MULT = 37
MULT_INV = 45
PLANE_MULT = 13
MESH = pl.DeviceIdType.MESH
BF = jnp.bfloat16
F32 = jnp.float32


def dot(a, b):
    return lax.dot_general(a, b, (((1,), (0,)), ((), ())), preferred_element_type=F32)


def dot_nt(a, b):
    return lax.dot_general(a, b, (((1,), (1,)), ((), ())), preferred_element_type=F32)


def dot_tn(a, b):
    return lax.dot_general(a, b, (((0,), (0,)), ((), ())), preferred_element_type=F32)


def rem(a, n):
    return lax.rem(a, jnp.int32(n))


def div(a, n):
    return lax.div(a, jnp.int32(n))


def offsets(i):
    k = rem(i * MULT, DEV)
    return div(k, 32), rem(div(k, 8), 4), rem(div(k, 2), 4), rem(k, 2)


def index_of(z, x, y, c):
    return rem(z, 4), rem(x, 4) * 8 + rem(y, 4) * 2 + rem(c, 2)


def mega(
    scale,
    stream_h, cot_h, gain_h, index_h, gates_h, wg_h, wu_h, wd_h, q_h, k_h, v_h,
    rows_o, gout_o, hid_o, dpre_o, router_o, g_o, gq_o, gk_o, gv_o, gain_o,
    stream, cot, gain, index, gates, wg, wu, wd, qv, kv, vv,
    normed, xin, tindex, code, p8, send, recv, acc, rows, dy, gout, ghid, hid, dpre, rowst, hidt, stacked,
    wgt, wut, wdt, rsend, rrecv,
    gin, g, qt, skv, sqg, kv1, kvs, kv2, qg1, qgs, qg2, mixb, pk, pv, gq, gk, gv, gpart, gland, router,
    lsem, osem, fsem, frsem, bsem, brsem, asem, arsem, gsem, grsem, zsem,
):
    z = lax.axis_index("grp")
    s = lax.axis_index("seq")
    x, y, c = div(s, 8), rem(div(s, 2), 4), rem(s, 2)

    def dev(z2, s2):
        return {"grp": z2, "seq": s2}

    def out_to(i):
        dz, dx, dy, dc = offsets(i)
        return dev(*index_of(z + dz, x + dx, y + dy, c + dc))

    def back_to(i):
        dz, dx, dy, dc = offsets(i)
        return dev(*index_of(z + 4 - dz, x + 4 - dx, y + 4 - dy, c + dc))

    def plane_to(j):
        k = rem(j * PLANE_MULT, PLANE)
        return index_of(z, x + div(k, 8), y + rem(div(k, 2), 4), c + rem(k, 2))[1]

    bar = pltpu.get_barrier_semaphore()

    def greet(j, carry):
        pl.semaphore_signal(bar, inc=1, device_id=dev(z, plane_to(j)), device_id_type=MESH)
        return carry

    lax.fori_loop(1, PLANE, greet, 0)
    for d in (1, 2, 3):
        pl.semaphore_signal(bar, inc=1, device_id=dev(rem(z + d, 4), s), device_id_type=MESH)

    loads = [
        (index_h, index), (stream_h, stream), (cot_h, cot), (gain_h, gain),
        (gates_h, gates), (q_h, qv), (k_h, kv), (v_h, vv), (wg_h, wg), (wu_h, wu), (wd_h, wd),
    ]
    load = [pltpu.make_async_copy(a, b, lsem.at[n]) for n, (a, b) in enumerate(loads)]
    for cp in load:
        cp.start()

    load[0].wait()
    here = z * PLANE + s
    tindex[...] = (index[...] - here * TOK).astype(F32).T
    token = lax.broadcasted_iota(jnp.int32, (TOK, DEV), 0).astype(F32)

    def match(n, found):
        eight = tindex[pl.ds(pl.multiple_of(n * 8, 8), 8), :]
        for r in range(8):
            found = jnp.where(eight[r:r + 1, :] == token, 1.0, found)
        return found

    found = lax.fori_loop(0, CAP // 8, match, jnp.zeros((TOK, DEV), F32))
    earlier = lax.broadcasted_iota(jnp.int32, (TOK, TOK), 0) > lax.broadcasted_iota(jnp.int32, (TOK, TOK), 1)
    before = dot(jnp.where(earlier, 1.0, 0.0).astype(BF), found.astype(BF))
    code[...] = (found * (before + 1.0)).astype(BF)

    pl.semaphore_wait(bar, PLANE - 1 + 3)
    for d in (1, 2, 3):
        pl.semaphore_signal(zsem, inc=1, device_id=dev(rem(z + d, 4), s), device_id_type=MESH)

    def build(gi, carry):
        r = lax.broadcasted_iota(jnp.int32, (256, 128), 0) + gi * 256
        lane = lax.broadcasted_iota(jnp.int32, (256, 128), 1)
        k = ((r >> 3) * MULT) & (DEV - 1)
        e = ((z + (k >> 5)) & 3) * 32 + ((x + (k >> 3)) & 3) * 8 + ((y + (k >> 1)) & 3) * 2 + ((c + k) & 1)
        pick = jnp.where(e == lane, 1.0, 0.0).astype(BF)
        rep = dot_nt(pick, code[...])
        want = ((r & 3) + 1).astype(F32)
        hit = jnp.where(rep == want, 1.0, 0.0)
        half = (r >> 2) & 1
        row0 = pl.multiple_of(gi * 256, 256)
        p8[pl.ds(row0, 256), 0:128] = jnp.where(half == 0, hit, 0.0).astype(BF)
        p8[pl.ds(row0, 256), 128:256] = jnp.where(half == 1, hit, 0.0).astype(BF)
        return carry

    lax.fori_loop(0, 4, build, 0)

    def fold(o):
        o = o.reshape(32, 8, 1024)
        return jnp.concatenate([o[:, :, 0:512], o[:, :, 512:1024]], axis=1).astype(BF)

    def fill(kind):
        def one(gi, carry):
            row0 = pl.multiple_of(gi * 256, 256)
            send[kind, pl.ds(gi * 32, 32)] = fold(dot(p8[pl.ds(row0, 256), :], xin[kind]))
            return carry

        lax.fori_loop(0, 4, one, 0)

    def push(kind):
        def one(i, carry):
            pltpu.make_async_remote_copy(
                send.at[kind, i], recv.at[kind, i], fsem.at[kind], frsem.at[kind, div(i, 32)],
                device_id=out_to(i), device_id_type=MESH,
            ).start()
            return carry

        lax.fori_loop(1, DEV, one, 0)
        recv[kind, 0] = send[kind, 0]

    load[2].wait()
    xin[0, 0:TOK, :] = cot[:, 0:1024]
    xin[0, TOK:, :] = cot[:, 1024:]
    fill(0)
    pl.semaphore_wait(zsem, 3)
    push(0)

    load[1].wait()
    load[3].wait()
    wide = stream[...].astype(F32)
    inv = lax.rsqrt(jnp.mean(wide * wide, axis=1, keepdims=True) + EPS)
    nrm = wide * inv
    normed[...] = nrm
    xin[1, 0:TOK, :] = (nrm * gain[...])[:, 0:1024].astype(BF)
    xin[1, TOK:, :] = (nrm * gain[...])[:, 1024:].astype(BF)
    fill(1)
    push(1)

    for n in (4, 5, 6, 7):
        load[n].wait()
    tril = lax.broadcasted_iota(jnp.int32, (TOK, TOK), 0) >= lax.broadcasted_iota(jnp.int32, (TOK, TOK), 1)

    def head(h):
        return pl.ds(pl.multiple_of(h * HEAD, HEAD), HEAD)

    def local_kv(h, carry):
        kh = kv[:, head(h)]
        skv[pl.ds(2 * h, 2)] = dot_tn(kh, vv[:, head(h)]).reshape(2, 64, HEAD).astype(BF)
        qt[head(h), :] = qv[:, head(h)].T
        mixb[h] = jnp.where(tril, dot_nt(qv[:, head(h)], kh), 0.0).astype(BF)
        return carry

    lax.fori_loop(0, HEADS, local_kv, 0)

    def scatter(src, dst, sem, rsem):
        def one(j, carry):
            to = plane_to(j)
            pltpu.make_async_remote_copy(
                src.at[to], dst.at[s], sem, rsem, device_id=dev(z, to), device_id_type=MESH
            ).start()
            return carry

        lax.fori_loop(1, PLANE, one, 0)
        dst[s] = src[s]

    def arrived(dst, rsem):
        span = dst.at[pl.ds(0, PLANE - 1)]
        pltpu.make_async_copy(span, span, rsem).wait()

    scatter(skv, kv1, asem.at[0], arsem.at[0])

    own_row = index[pl.ds(here, 1), :]
    own_col = jnp.broadcast_to(own_row.astype(F32), (8, CAP)).T[:, 0:1].astype(jnp.int32)
    wide_row = jnp.broadcast_to(own_row, (CAP, CAP))
    wide_col = jnp.broadcast_to(own_col, (CAP, CAP))
    mate = (wide_row >> 7) == (wide_col >> 7)
    slot_col = jnp.sum(jnp.where(mate & (wide_row < wide_col), 1.0, 0.0), axis=1, keepdims=True)
    slot_row = jnp.sum(jnp.where(mate & (wide_col < wide_row), 1.0, 0.0), axis=0, keepdims=True)

    def place(own, slot):
        src = own >> 7
        k = (
            ((z - (src >> 5)) & 3) * 32 + ((x - (src >> 3)) & 3) * 8 + ((y - (src >> 1)) & 3) * 2 + ((c - src) & 1)
        )
        return ((k * MULT_INV) & (DEV - 1)) * 8 + slot.astype(jnp.int32)

    at_col = place(own_col, slot_col)
    at_row = place(own_row, slot_row)
    tcol = jnp.concatenate([at_col, at_col + 4], axis=0)
    trow = jnp.concatenate([at_row, at_row + 4], axis=1)
    gate_col = jnp.broadcast_to(gates[...], (8, CAP)).T[:, 0:1]

    for n in (8, 9, 10):
        load[n].wait()

    def turn_weights(n, carry):
        c0 = pl.multiple_of(n * 256, 256)
        wgt[:, pl.ds(c0, 256)] = wg[pl.ds(c0, 256), :].T
        wut[:, pl.ds(c0, 256)] = wu[pl.ds(c0, 256), :].T
        wdt[pl.ds(c0, 256), :] = wd[:, pl.ds(c0, 256)].T
        return carry

    lax.fori_loop(0, 8, turn_weights, 0)

    def settle(kind, dst):
        for gi in range(4):
            first = 1 if gi == 0 else 0
            span = recv.at[kind, pl.ds(gi * 32 + first, 32 - first)]
            pltpu.make_async_copy(span, span, frsem.at[kind, gi]).wait()
            lane = lax.broadcasted_iota(jnp.int32, (512, 256), 1) + gi * 256
            put = jnp.where(lane == tcol, 1.0, 0.0).astype(BF)
            for half in range(2):
                f = recv[kind, pl.ds(gi * 32, 32)].astype(F32).reshape(32, 2, 8, 512)[:, half]
                part = dot(put, f.reshape(256, 512).astype(BF))
                at = slice(half * 512, (half + 1) * 512)
                if gi == 0:
                    acc[:, at] = part
                elif gi < 3:
                    acc[:, at] += part
                else:
                    part = (acc[:, at] + part).astype(BF)
                    dst[:, half * 512:(half + 1) * 512] = part[0:CAP]
                    dst[:, 1024 + half * 512:1024 + (half + 1) * 512] = part[CAP:]

    settle(0, dy)
    gout[...] = (gate_col * dy[...].astype(F32)).astype(BF)
    ghid[...] = dot(gout[...], wdt[...])
    settle(1, rows)

    def front(n, carry):
        c0 = pl.multiple_of(n * 256, 256)
        gp = dot(rows[...], wg[:, pl.ds(c0, 256)])
        up = dot(rows[...], wu[:, pl.ds(c0, 256)])
        gh = ghid[:, pl.ds(c0, 256)]
        sg = jax.nn.sigmoid(gp)
        silu = gp * sg
        hid[:, pl.ds(c0, 256)] = (silu * up).astype(BF)
        dpre[:, pl.ds(c0, 256)] = (gh * up * (sg * (1.0 + gp * (1.0 - sg)))).astype(BF)
        dpre[:, pl.ds(pl.multiple_of(c0 + FF, 256), 256)] = (gh * silu).astype(BF)
        return carry

    lax.fori_loop(0, 3, front, 0)

    def back(n, carry):
        r0 = pl.multiple_of(n * 256, 256)
        gr = dot(dpre[:, 0:FF], wgt[:, pl.ds(r0, 256)]) + dot(dpre[:, FF:], wut[:, pl.ds(r0, 256)])
        h0 = pl.multiple_of(div(n, 4) * 256, 256)
        c0 = pl.multiple_of(rem(n, 4) * 256, 256)
        stacked[pl.ds(h0, 256), pl.ds(c0, 256)] = gr.astype(BF)
        return carry

    lax.fori_loop(0, 8, back, 0)

    def refill(gi, carry):
        r = lax.broadcasted_iota(jnp.int32, (256, 512), 0) + gi * 256
        put = jnp.where(r == trow, 1.0, 0.0).astype(BF)
        rsend[pl.ds(gi * 32, 32)] = fold(dot(put, stacked[...]))
        return carry

    def ret(i, carry):
        pltpu.make_async_remote_copy(
            rsend.at[i], rrecv.at[i], bsem, brsem.at[div(i, 32)], device_id=back_to(i), device_id_type=MESH
        ).start()
        return carry

    lax.fori_loop(0, 2, refill, 0)
    lax.fori_loop(1, 32, ret, 0)
    lax.fori_loop(2, 3, refill, 0)
    lax.fori_loop(32, 64, ret, 0)
    lax.fori_loop(3, 4, refill, 0)
    lax.fori_loop(64, 128, ret, 0)
    rrecv[0] = rsend[0]

    def turn(n, carry):
        c0 = pl.multiple_of(n * 256, 256)
        rowst[pl.ds(c0, 256), :] = rows[:, pl.ds(c0, 256)].T
        return carry

    lax.fori_loop(0, 8, turn, 0)
    for n in range(3):
        hidt[n * 256:(n + 1) * 256, :] = hid[:, n * 256:(n + 1) * 256].T
    outs = [(rowst, rows_o), (gout, gout_o), (hidt, hid_o), (dpre, dpre_o)]
    store = [pltpu.make_async_copy(a, b, osem.at[n]) for n, (a, b) in enumerate(outs)]
    for cp in store:
        cp.start()

    def route(n, total):
        c0 = pl.multiple_of(n * 256, 256)
        eo = dot(hid[...], wd[:, pl.ds(c0, 256)])
        return total + jnp.sum(dy[:, pl.ds(c0, 256)].astype(F32) * eo, axis=1, keepdims=True)

    router_col = lax.fori_loop(0, 8, route, jnp.zeros((CAP, 1), F32))
    router[...] = jnp.broadcast_to(router_col, (CAP, 128)).T[0:1, :]

    arrived(kv1, arsem.at[0])

    def prefix(r, total):
        kvs[r] = total.astype(BF)
        return total + kv1[r].astype(F32)

    lax.fori_loop(0, PLANE, prefix, jnp.zeros((64, HEAD), F32))
    scatter(kvs, kv2, asem.at[1], arsem.at[1])

    for gi in range(4):
        first = 1 if gi == 0 else 0
        span = rrecv.at[pl.ds(gi * 32 + first, 32 - first)]
        pltpu.make_async_copy(span, span, brsem.at[gi]).wait()
        for half in range(2):
            f = rrecv[pl.ds(gi * 32, 32)].astype(F32).reshape(32, 2, 8, 512)[:, half]
            f = f.reshape(256, 512).astype(BF)
            part = dot_tn(p8[gi * 256:(gi + 1) * 256, :], f)
            for hh in range(2):
                c0 = hh * 1024 + half * 512
                piece = part[hh * TOK:(hh + 1) * TOK, :]
                if gi == 0:
                    gin[:, c0:c0 + 512] = piece
                else:
                    gin[:, c0:c0 + 512] += piece

    gi_ = gin[...]
    nrm = normed[...]

    def spread(stage):
        if stage == 0:
            to = [dev(z, s + 1 - 2 * c)]
        elif stage == 1:
            to = [dev(z, x * 8 + rem(y + d, 4) * 2 + c) for d in (1, 2, 3)]
        elif stage == 2:
            to = [dev(z, rem(x + d, 4) * 8 + y * 2 + c) for d in (1, 2, 3)]
        else:
            to = [dev(rem(z + d, 4), s) for d in (1, 2, 3)]
        cps = [
            pltpu.make_async_remote_copy(
                gpart.at[stage], gland.at[stage, d], gsem.at[stage, d], grsem.at[stage, d],
                device_id=t, device_id_type=MESH,
            )
            for d, t in enumerate(to)
        ]
        for cp in cps:
            cp.start()
        return cps

    def collect(stage, cps):
        for cp in cps:
            cp.wait()
        total = gpart[stage]
        for d in range(len(cps)):
            total = total + gland[stage, d]
        return total

    gpart[0] = jnp.sum(gi_ * nrm, axis=0, keepdims=True)
    cps0 = spread(0)

    gn = gi_ * gain[...]
    wide_g = cot[...].astype(F32) + inv * (gn - nrm * jnp.mean(gn * nrm, axis=1, keepdims=True))
    g[...] = wide_g.astype(BF)
    gcp = pltpu.make_async_copy(g, g_o, osem.at[4])
    gcp.start()
    for h in range(HEADS):
        at = slice(h * HEAD, (h + 1) * HEAD)
        sqg[2 * h:2 * h + 2] = dot(qt[at, :], g[:, at]).reshape(2, 64, HEAD).astype(BF)
    scatter(sqg, qg1, asem.at[2], arsem.at[2])
    gpart[1] = collect(0, cps0)
    cps1 = spread(1)

    def local_terms(h, carry):
        gh = g[:, head(h)]
        mix_a = jnp.where(tril, dot_nt(gh, vv[:, head(h)]), 0.0).astype(BF)
        gin[:, head(h)] = dot(mix_a, kv[:, head(h)])
        pk[:, head(h)] = dot_tn(mix_a, qv[:, head(h)])
        pv[:, head(h)] = dot_tn(mixb[h], gh)
        return carry

    lax.fori_loop(0, HEADS, local_terms, 0)
    arrived(qg1, arsem.at[2])

    def suffix(n, total):
        r = PLANE - 1 - n
        qgs[r] = total.astype(BF)
        return total + qg1[r].astype(F32)

    lax.fori_loop(0, PLANE, suffix, jnp.zeros((64, HEAD), F32))
    scatter(qgs, qg2, asem.at[3], arsem.at[3])
    gpart[2] = collect(1, cps1)
    cps2 = spread(2)
    arrived(kv2, arsem.at[1])

    def early_terms(h, carry):
        prior = kv2[pl.ds(2 * h, 2)].reshape(HEAD, HEAD)
        gq[:, head(h)] = (scale * (gin[:, head(h)] + dot_nt(g[:, head(h)], prior))).astype(BF)
        return carry

    lax.fori_loop(0, HEADS, early_terms, 0)
    late = [pltpu.make_async_copy(gq, gq_o, osem.at[5])]
    late[0].start()
    gpart[3] = collect(2, cps2)
    cps3 = spread(3)
    arrived(qg2, arsem.at[3])
    for h in range(HEADS):
        at = slice(h * HEAD, (h + 1) * HEAD)
        later = qg2[2 * h:2 * h + 2].reshape(HEAD, HEAD)
        gk[:, at] = (scale * (pk[:, at] + dot_nt(vv[:, at], later))).astype(BF)
        gv[:, at] = (scale * (pv[:, at] + dot(kv[:, at], later))).astype(BF)
    gpart[4] = collect(3, cps3)
    for n, (a, b) in enumerate([(gk, gk_o), (gv, gv_o), (gpart.at[4], gain_o), (router, router_o)]):
        late.append(pltpu.make_async_copy(a, b, osem.at[6 + n]))
        late[-1].start()

    for kind in (0, 1):
        span = send.at[kind, pl.ds(1, DEV - 1)]
        pltpu.make_async_copy(span, span, fsem.at[kind]).wait()
    span = rsend.at[pl.ds(1, DEV - 1)]
    pltpu.make_async_copy(span, span, bsem).wait()
    for n, buf in enumerate((skv, kvs, sqg, qgs)):
        arrived(buf, asem.at[n])
    for cp in store + [gcp] + late:
        cp.wait()


def call_mega(scale, operands):
    def vm(shape, dtype):
        return pltpu.VMEM(shape, dtype)

    state = (PLANE, 64, HEAD)
    results = [
        ((D, CAP), BF), ((CAP, D), BF), ((FF, CAP), BF), ((CAP, 2 * FF), BF), ((1, CAP), F32),
        ((TOK, D), BF), ((TOK, D), BF), ((TOK, D), BF), ((TOK, D), BF), ((1, D), F32),
    ]
    scratch = [
        vm((TOK, D), BF), vm((TOK, D), BF), vm((1, D), F32), vm((DEV, CAP), jnp.int32), vm((1, CAP), F32),
        vm((D, FF), BF), vm((D, FF), BF), vm((FF, D), BF),
        vm((TOK, D), BF), vm((TOK, D), BF), vm((TOK, D), BF),
        vm((TOK, D), F32), vm((2, 256, 1024), BF), vm((CAP, DEV), F32), vm((TOK, DEV), BF), vm((1024, 256), BF),
        vm((2, DEV, 16, 512), BF), vm((2, DEV, 16, 512), BF), vm((512, 1024), F32), vm((CAP, D), BF),
        vm((CAP, D), BF), vm((CAP, D), BF), vm((CAP, FF), F32), vm((CAP, FF), BF), vm((CAP, 2 * FF), BF),
        vm((D, CAP), BF), vm((FF, CAP), BF), vm((512, 1024), BF),
        vm((FF, D), BF), vm((FF, D), BF), vm((D, FF), BF),
        vm((DEV, 16, 512), BF), vm((DEV, 16, 512), BF),
        vm((TOK, D), F32), vm((TOK, D), BF),
        vm((D, TOK), BF),
    ] + [vm(state, BF)] * 8 + [
        vm((HEADS, HEAD, HEAD), BF), vm((TOK, D), F32), vm((TOK, D), F32),
        vm((TOK, D), BF), vm((TOK, D), BF), vm((TOK, D), BF),
        vm((5, 1, D), F32), vm((4, 3, 1, D), F32), vm((1, CAP), F32),
    ]
    dma = pltpu.SemaphoreType.DMA
    sems = [
        dma((11,)), dma((10,)), dma((2,)), dma((2, 4)), dma, dma((4,)), dma((4,)), dma((4,)), dma((4, 3)), dma((4, 3)),
        pltpu.SemaphoreType.REGULAR,
    ]
    return pl.pallas_call(
        functools.partial(mega, scale),
        out_shape=[jax.ShapeDtypeStruct(a, b) for a, b in results],
        in_specs=[pl.BlockSpec(memory_space=pl.ANY)] * 11,
        out_specs=[pl.BlockSpec(memory_space=pl.ANY)] * len(results),
        scratch_shapes=scratch + sems,
        compiler_params=pltpu.CompilerParams(
            collective_id=0, has_side_effects=True, vmem_limit_bytes=63 * 1024 * 1024
        ),
        name="mega",
    )(*operands)


def finish(
    rowst_h, gout_h, hidt_h, dpre_h, router_h, g_h, gq_h, gk_h, gv_h, gain_h,
    gate_o, up_o, down_o, router_o, g_o, gq_o, gk_o, gv_o, gain_o,
    rowst, gout, hidt, dpre, router, g, gq, gk, gv, gain, gate, up, down, lsem, psem, wsem,
):
    ins = [(hidt_h, hidt), (gout_h, gout), (rowst_h, rowst), (dpre_h, dpre)]
    loads = [pltpu.make_async_copy(a, b, lsem.at[n]) for n, (a, b) in enumerate(ins)]
    through = [(g_h, g, g_o), (gq_h, gq, gq_o), (gk_h, gk, gk_o), (gv_h, gv, gv_o), (router_h, router, router_o),
               (gain_h, gain, gain_o)]
    take = [pltpu.make_async_copy(a, b, lsem.at[4 + n]) for n, (a, b, o) in enumerate(through)]
    give = [pltpu.make_async_copy(b, o, psem.at[n]) for n, (a, b, o) in enumerate(through)]
    for cp in loads + take:
        cp.start()
    writes = []

    def put(src, dst, rows):
        cp = pltpu.make_async_copy(src.at[rows], dst.at[rows], wsem.at[len(writes)])
        cp.start()
        writes.append(cp)

    loads[0].wait()
    loads[1].wait()
    for n in range(3):
        r = pl.ds(n * 256, 256)
        for m in range(2):
            col = pl.ds(m * 1024, 1024)
            down[r, col] = dot(hidt[r, :], gout[:, col]).astype(BF)
        put(down, down_o, r)
    loads[2].wait()
    loads[3].wait()
    for n in range(8):
        r = pl.ds(n * 256, 256)
        gate[r, :] = dot(rowst[r, :], dpre[:, 0:FF]).astype(BF)
        put(gate, gate_o, r)
        up[r, :] = dot(rowst[r, :], dpre[:, FF:]).astype(BF)
        put(up, up_o, r)
        if n < len(through):
            take[n].wait()
            give[n].start()
    for cp in give + writes:
        cp.wait()


def call_finish(operands):
    def vm(shape, dtype):
        return pltpu.VMEM(shape, dtype)

    small = [((1, CAP), F32), ((TOK, D), BF), ((TOK, D), BF), ((TOK, D), BF), ((TOK, D), BF), ((1, D), F32)]
    weights = [((D, FF), BF), ((D, FF), BF), ((FF, D), BF)]
    dma = pltpu.SemaphoreType.DMA
    return pl.pallas_call(
        finish,
        out_shape=[jax.ShapeDtypeStruct(a, b) for a, b in weights + small],
        in_specs=[pl.BlockSpec(memory_space=pl.ANY)] * 10,
        out_specs=[pl.BlockSpec(memory_space=pl.ANY)] * 9,
        scratch_shapes=[vm((D, CAP), BF), vm((CAP, D), BF), vm((FF, CAP), BF), vm((CAP, 2 * FF), BF)]
        + [vm(a, b) for a, b in small + weights]
        + [dma((10,)), dma((6,)), dma((19,))],
        compiler_params=pltpu.CompilerParams(vmem_limit_bytes=63 * 1024 * 1024),
        name="finish",
    )(*operands)


def body(stream, cotangent, norm_gain, queries, key_vectors, value_vectors, expert_index, router_gates,
         gate_proj, up_proj, down_proj):
    scale = 1.0 / math.sqrt(HEAD * TOK * PLANE)
    results = call_mega(scale, (
        stream, cotangent, norm_gain[None, :], expert_index, router_gates, gate_proj[0], up_proj[0], down_proj[0],
        queries, key_vectors, value_vectors,
    ))
    gate, up, down, router, g, gq, gk, gv, gain = call_finish(results)
    return (g, gq, gk, gv, gate[None], up[None], down[None], router, gain[0])


def solution(mesh):
    both = ("grp", "seq")
    r2, r3 = P(both, None), P(both, None, None)
    return jax.shard_map(
        body,
        mesh=mesh,
        in_specs=(r2, r2, P(), r2, r2, r2, P(), r2, r3, r3, r3),
        out_specs=(r2, r2, r2, r2, r3, r3, r3, r2, P()),
        check_vma=False,
    )
```

```python
import functools
import math

import jax
import jax.numpy as jnp
from jax import lax
from jax.experimental import pallas as pl
from jax.experimental.pallas import tpu as pltpu
from jax.sharding import PartitionSpec as P

D = 2048
FF = 768
HEADS = 16
HEAD = 128
CAP = 256
TOK = 128
DEV = 128
PLANE = 32
CHIPS = 16
CHIP_MULT = 7
SLOTS = 4
EPS = 1e-06
MULT = 91
MULT_INV = 83
PLANE_MULT = 13
MESH = pl.DeviceIdType.MESH
BF = jnp.bfloat16
F32 = jnp.float32


def dot(a, b):
    return lax.dot_general(a, b, (((1,), (0,)), ((), ())), preferred_element_type=F32)


def dot_nt(a, b):
    return lax.dot_general(a, b, (((1,), (1,)), ((), ())), preferred_element_type=F32)


def dot_tn(a, b):
    return lax.dot_general(a, b, (((0,), (0,)), ((), ())), preferred_element_type=F32)


def rem(a, n):
    return lax.rem(a, jnp.int32(n))


def div(a, n):
    return lax.div(a, jnp.int32(n))


def offsets(i):
    k = rem(i * MULT, DEV)
    return div(k, 32), rem(div(k, 8), 4), rem(div(k, 2), 4), rem(k, 2)


def index_of(z, x, y, c):
    return rem(z, 4), rem(x, 4) * 8 + rem(y, 4) * 2 + rem(c, 2)


def mega(
    scale,
    stream_h, cot_h, gain_h, index_h, gates_h, wg_h, wu_h, wd_h, q_h, k_h, v_h,
    rows_o, gout_o, hid_o, dpre_o, router_o, g_o, gq_o, gk_o, gv_o, gain_o,
    stream, cot, gain, index, gates, wg, wu, wd, qv, kv, vv,
    normed, xin, tindex, code, p8, send, recv, acc, rows, dy, gout, ghid, hid, dpre, rowst, hidt, stacked,
    wgt, wut, wdt, rsend, rrecv,
    gin, g, qt, skv, sqg, okv, oqg, kv2, qg2, tkv, kv1, kvs, tqg, qg1, qgs, mixb, pk, pv, gq, gk, gv, gpart, gland, router,
    lsem, osem, fsem, frsem, bsem, brsem, asem, arsem, wsem, wrsem, gsem, grsem, zsem,
):
    z = lax.axis_index("grp")
    s = lax.axis_index("seq")
    x, y, c = div(s, 8), rem(div(s, 2), 4), rem(s, 2)

    def dev(z2, s2):
        return {"grp": z2, "seq": s2}

    def out_to(i):
        dz, dx, dy, dc = offsets(i)
        return dev(*index_of(z + dz, x + dx, y + dy, c + dc))

    def back_to(i):
        dz, dx, dy, dc = offsets(i)
        return dev(*index_of(z + 4 - dz, x + 4 - dx, y + 4 - dy, c + dc))

    def plane_to(j):
        k = rem(j * PLANE_MULT, PLANE)
        return index_of(z, x + div(k, 8), y + rem(div(k, 2), 4), c + rem(k, 2))[1]

    bar = pltpu.get_barrier_semaphore()

    def greet(j, carry):
        pl.semaphore_signal(bar, inc=1, device_id=dev(z, plane_to(j)), device_id_type=MESH)
        return carry

    lax.fori_loop(1, PLANE, greet, 0)
    for d in (1, 2, 3):
        pl.semaphore_signal(bar, inc=1, device_id=dev(rem(z + d, 4), s), device_id_type=MESH)

    loads = [
        (index_h, index), (stream_h, stream), (cot_h, cot), (gain_h, gain),
        (gates_h, gates), (q_h, qv), (k_h, kv), (v_h, vv), (wg_h, wg), (wu_h, wu), (wd_h, wd),
    ]
    load = [pltpu.make_async_copy(a, b, lsem.at[n]) for n, (a, b) in enumerate(loads)]
    for cp in load:
        cp.start()

    load[0].wait()
    here = z * PLANE + s
    tindex[...] = (index[...] - here * TOK).astype(F32).T
    token = lax.broadcasted_iota(jnp.int32, (TOK, DEV), 0).astype(F32)

    def match(n, found):
        eight = tindex[pl.ds(pl.multiple_of(n * 8, 8), 8), :]
        for r in range(8):
            found = jnp.where(eight[r:r + 1, :] == token, 1.0, found)
        return found

    found = lax.fori_loop(0, CAP // 8, match, jnp.zeros((TOK, DEV), F32))
    earlier = lax.broadcasted_iota(jnp.int32, (TOK, TOK), 0) > lax.broadcasted_iota(jnp.int32, (TOK, TOK), 1)
    before = dot(jnp.where(earlier, 1.0, 0.0).astype(BF), found.astype(BF))
    code[...] = (found * (before + 1.0)).astype(BF)

    pl.semaphore_wait(bar, PLANE - 1 + 3)
    for d in (1, 2, 3):
        pl.semaphore_signal(zsem, inc=1, device_id=dev(rem(z + d, 4), s), device_id_type=MESH)

    def build(gi, carry):
        r = lax.broadcasted_iota(jnp.int32, (256, 128), 0) + gi * 256
        lane = lax.broadcasted_iota(jnp.int32, (256, 128), 1)
        k = ((r >> 3) * MULT) & (DEV - 1)
        e = ((z + (k >> 5)) & 3) * 32 + ((x + (k >> 3)) & 3) * 8 + ((y + (k >> 1)) & 3) * 2 + ((c + k) & 1)
        pick = jnp.where(e == lane, 1.0, 0.0).astype(BF)
        rep = dot_nt(pick, code[...])
        want = ((r & 3) + 1).astype(F32)
        hit = jnp.where(rep == want, 1.0, 0.0)
        half = (r >> 2) & 1
        row0 = pl.multiple_of(gi * 256, 256)
        p8[pl.ds(row0, 256), 0:128] = jnp.where(half == 0, hit, 0.0).astype(BF)
        p8[pl.ds(row0, 256), 128:256] = jnp.where(half == 1, hit, 0.0).astype(BF)
        return carry

    lax.fori_loop(0, 4, build, 0)

    def fold(o):
        o = o.reshape(32, 8, 1024)
        return jnp.concatenate([o[:, :, 0:512], o[:, :, 512:1024]], axis=1).astype(BF)

    def fill(kind):
        def one(gi, carry):
            row0 = pl.multiple_of(gi * 256, 256)
            send[kind, pl.ds(gi * 32, 32)] = fold(dot(p8[pl.ds(row0, 256), :], xin[kind]))
            return carry

        lax.fori_loop(0, 4, one, 0)

    def push(kind):
        def one(i, carry):
            pltpu.make_async_remote_copy(
                send.at[kind, i], recv.at[kind, i], fsem.at[kind], frsem.at[kind, div(i, 32)],
                device_id=out_to(i), device_id_type=MESH,
            ).start()
            return carry

        lax.fori_loop(1, DEV, one, 0)
        recv[kind, 0] = send[kind, 0]

    load[2].wait()
    xin[0, 0:TOK, :] = cot[:, 0:1024]
    xin[0, TOK:, :] = cot[:, 1024:]
    fill(0)
    pl.semaphore_wait(zsem, 3)
    push(0)

    load[1].wait()
    load[3].wait()
    wide = stream[...].astype(F32)
    inv = lax.rsqrt(jnp.mean(wide * wide, axis=1, keepdims=True) + EPS)
    nrm = wide * inv
    normed[...] = nrm
    xin[1, 0:TOK, :] = (nrm * gain[...])[:, 0:1024].astype(BF)
    xin[1, TOK:, :] = (nrm * gain[...])[:, 1024:].astype(BF)
    fill(1)
    push(1)

    for n in (4, 5, 6, 7):
        load[n].wait()
    tril = lax.broadcasted_iota(jnp.int32, (TOK, TOK), 0) >= lax.broadcasted_iota(jnp.int32, (TOK, TOK), 1)

    def head(h):
        return pl.ds(pl.multiple_of(h * HEAD, HEAD), HEAD)

    def local_kv(h, carry):
        kh = kv[:, head(h)]
        skv[pl.ds(2 * h, 2)] = dot_tn(kh, vv[:, head(h)]).reshape(2, 64, HEAD).astype(BF)
        qt[head(h), :] = qv[:, head(h)].T
        mixb[h] = jnp.where(tril, dot_nt(qv[:, head(h)], kh), 0.0).astype(BF)
        return carry

    lax.fori_loop(0, HEADS, local_kv, 0)

    chip = x * 4 + y
    mine = pl.ds(c * CHIPS, CHIPS)
    theirs = pl.ds((1 - c) * CHIPS, CHIPS)

    def swap(src, dst, part, n):
        cp = pltpu.make_async_remote_copy(
            src.at[part], dst.at[part], wsem.at[n], wrsem.at[n], device_id=dev(z, s + 1 - 2 * c), device_id_type=MESH
        )
        cp.start()
        return cp

    def landed(dst, part, n):
        span = dst.at[part]
        pltpu.make_async_copy(span, span, wrsem.at[n]).wait()

    def scatter(src, dst, base, at, n):
        def one(j, carry):
            k = rem(j * CHIP_MULT, CHIPS)
            x2, y2 = rem(x + div(k, 4), 4), rem(y + rem(k, 4), 4)
            pltpu.make_async_remote_copy(
                src.at[x2 * 4 + y2], dst.at[base + at], asem.at[n], arsem.at[n],
                device_id=dev(z, x2 * 8 + y2 * 2 + c), device_id_type=MESH,
            ).start()
            return carry

        lax.fori_loop(1, CHIPS, one, 0)
        dst[base + at] = src[at]

    def arrived(dst, sem):
        span = dst.at[pl.ds(0, CHIPS - 1)]
        pltpu.make_async_copy(span, span, sem).wait()

    swaps = [swap(skv, okv, theirs, 0), swap(skv, okv, mine, 1)]

    own_row = index[pl.ds(here, 1), :]
    own_col = jnp.broadcast_to(own_row.astype(F32), (8, CAP)).T[:, 0:1].astype(jnp.int32)
    wide_row = jnp.broadcast_to(own_row, (CAP, CAP))
    wide_col = jnp.broadcast_to(own_col, (CAP, CAP))
    mate = (wide_row >> 7) == (wide_col >> 7)
    slot_col = jnp.sum(jnp.where(mate & (wide_row < wide_col), 1.0, 0.0), axis=1, keepdims=True)
    slot_row = jnp.sum(jnp.where(mate & (wide_col < wide_row), 1.0, 0.0), axis=0, keepdims=True)

    def place(own, slot):
        src = own >> 7
        k = (
            ((z - (src >> 5)) & 3) * 32 + ((x - (src >> 3)) & 3) * 8 + ((y - (src >> 1)) & 3) * 2 + ((c - src) & 1)
        )
        return ((k * MULT_INV) & (DEV - 1)) * 8 + slot.astype(jnp.int32)

    at_col = place(own_col, slot_col)
    at_row = place(own_row, slot_row)
    tcol = jnp.concatenate([at_col, at_col + 4], axis=0)
    trow = jnp.concatenate([at_row, at_row + 4], axis=1)
    gate_col = jnp.broadcast_to(gates[...], (8, CAP)).T[:, 0:1]

    for n in (8, 9, 10):
        load[n].wait()

    def turn_weights(n, carry):
        c0 = pl.multiple_of(n * 256, 256)
        wgt[:, pl.ds(c0, 256)] = wg[pl.ds(c0, 256), :].T
        wut[:, pl.ds(c0, 256)] = wu[pl.ds(c0, 256), :].T
        wdt[pl.ds(c0, 256), :] = wd[:, pl.ds(c0, 256)].T
        return carry

    lax.fori_loop(0, 8, turn_weights, 0)
    landed(okv, mine, 0)
    tkv[...] = (skv[mine].astype(F32) + okv[mine].astype(F32)).astype(BF)
    scatter(tkv, kv1, 0, chip, 0)

    def settle(kind, dst):
        for gi in range(4):
            first = 1 if gi == 0 else 0
            span = recv.at[kind, pl.ds(gi * 32 + first, 32 - first)]
            pltpu.make_async_copy(span, span, frsem.at[kind, gi]).wait()
            lane = lax.broadcasted_iota(jnp.int32, (512, 256), 1) + gi * 256
            put = jnp.where(lane == tcol, 1.0, 0.0).astype(BF)
            for half in range(2):
                f = recv[kind, pl.ds(gi * 32, 32)].astype(F32).reshape(32, 2, 8, 512)[:, half]
                part = dot(put, f.reshape(256, 512).astype(BF))
                at = slice(half * 512, (half + 1) * 512)
                if gi == 0:
                    acc[:, at] = part
                elif gi < 3:
                    acc[:, at] += part
                else:
                    part = (acc[:, at] + part).astype(BF)
                    dst[:, half * 512:(half + 1) * 512] = part[0:CAP]
                    dst[:, 1024 + half * 512:1024 + (half + 1) * 512] = part[CAP:]

    settle(0, dy)
    gout[...] = (gate_col * dy[...].astype(F32)).astype(BF)
    ghid[...] = dot(gout[...], wdt[...])
    settle(1, rows)

    def front(n, carry):
        c0 = pl.multiple_of(n * 256, 256)
        gp = dot(rows[...], wg[:, pl.ds(c0, 256)])
        up = dot(rows[...], wu[:, pl.ds(c0, 256)])
        gh = ghid[:, pl.ds(c0, 256)]
        sg = jax.nn.sigmoid(gp)
        silu = gp * sg
        hid[:, pl.ds(c0, 256)] = (silu * up).astype(BF)
        dpre[:, pl.ds(c0, 256)] = (gh * up * (sg * (1.0 + gp * (1.0 - sg)))).astype(BF)
        dpre[:, pl.ds(pl.multiple_of(c0 + FF, 256), 256)] = (gh * silu).astype(BF)
        return carry

    lax.fori_loop(0, 3, front, 0)

    def back(n, carry):
        r0 = pl.multiple_of(n * 256, 256)
        gr = dot(dpre[:, 0:FF], wgt[:, pl.ds(r0, 256)]) + dot(dpre[:, FF:], wut[:, pl.ds(r0, 256)])
        h0 = pl.multiple_of(div(n, 4) * 256, 256)
        c0 = pl.multiple_of(rem(n, 4) * 256, 256)
        stacked[pl.ds(h0, 256), pl.ds(c0, 256)] = gr.astype(BF)
        return carry

    lax.fori_loop(0, 8, back, 0)

    def refill(gi, carry):
        r = lax.broadcasted_iota(jnp.int32, (256, 512), 0) + gi * 256
        put = jnp.where(r == trow, 1.0, 0.0).astype(BF)
        rsend[pl.ds(gi * 32, 32)] = fold(dot(put, stacked[...]))
        return carry

    def ret(i, carry):
        pltpu.make_async_remote_copy(
            rsend.at[i], rrecv.at[i], bsem, brsem.at[div(i, 32)], device_id=back_to(i), device_id_type=MESH
        ).start()
        return carry

    lax.fori_loop(0, 2, refill, 0)
    lax.fori_loop(1, 32, ret, 0)
    lax.fori_loop(2, 3, refill, 0)
    lax.fori_loop(32, 64, ret, 0)
    lax.fori_loop(3, 4, refill, 0)
    lax.fori_loop(64, 128, ret, 0)
    rrecv[0] = rsend[0]

    def turn(n, carry):
        c0 = pl.multiple_of(n * 256, 256)
        rowst[pl.ds(c0, 256), :] = rows[:, pl.ds(c0, 256)].T
        return carry

    lax.fori_loop(0, 8, turn, 0)
    for n in range(3):
        hidt[n * 256:(n + 1) * 256, :] = hid[:, n * 256:(n + 1) * 256].T
    outs = [(rowst, rows_o), (gout, gout_o), (hidt, hid_o), (dpre, dpre_o)]
    store = [pltpu.make_async_copy(a, b, osem.at[n]) for n, (a, b) in enumerate(outs)]
    for cp in store:
        cp.start()

    def route(n, total):
        c0 = pl.multiple_of(n * 256, 256)
        eo = dot(hid[...], wd[:, pl.ds(c0, 256)])
        return total + jnp.sum(dy[:, pl.ds(c0, 256)].astype(F32) * eo, axis=1, keepdims=True)

    router_col = lax.fori_loop(0, 8, route, jnp.zeros((CAP, 1), F32))
    router[...] = jnp.broadcast_to(router_col, (CAP, 128)).T[0:1, :]

    arrived(kv1, arsem.at[0])

    def prefix(r, total):
        kvs[r] = total.astype(BF)
        return total + kv1[r].astype(F32)

    lax.fori_loop(0, CHIPS, prefix, jnp.zeros((64, HEAD), F32))
    scatter(kvs, kv2, c * CHIPS, chip, 1)

    for gi in range(4):
        first = 1 if gi == 0 else 0
        span = rrecv.at[pl.ds(gi * 32 + first, 32 - first)]
        pltpu.make_async_copy(span, span, brsem.at[gi]).wait()
        for half in range(2):
            f = rrecv[pl.ds(gi * 32, 32)].astype(F32).reshape(32, 2, 8, 512)[:, half]
            f = f.reshape(256, 512).astype(BF)
            part = dot_tn(p8[gi * 256:(gi + 1) * 256, :], f)
            for hh in range(2):
                c0 = hh * 1024 + half * 512
                piece = part[hh * TOK:(hh + 1) * TOK, :]
                if gi == 0:
                    gin[:, c0:c0 + 512] = piece
                else:
                    gin[:, c0:c0 + 512] += piece

    gi_ = gin[...]
    nrm = normed[...]

    def spread(stage):
        if stage == 0:
            to = [dev(z, s + 1 - 2 * c)]
        elif stage == 1:
            to = [dev(z, x * 8 + rem(y + d, 4) * 2 + c) for d in (1, 2, 3)]
        elif stage == 2:
            to = [dev(z, rem(x + d, 4) * 8 + y * 2 + c) for d in (1, 2, 3)]
        else:
            to = [dev(rem(z + d, 4), s) for d in (1, 2, 3)]
        cps = [
            pltpu.make_async_remote_copy(
                gpart.at[stage], gland.at[stage, d], gsem.at[stage, d], grsem.at[stage, d],
                device_id=t, device_id_type=MESH,
            )
            for d, t in enumerate(to)
        ]
        for cp in cps:
            cp.start()
        return cps

    def collect(stage, cps):
        for cp in cps:
            cp.wait()
        total = gpart[stage]
        for d in range(len(cps)):
            total = total + gland[stage, d]
        return total

    gpart[0] = jnp.sum(gi_ * nrm, axis=0, keepdims=True)
    cps0 = spread(0)

    gn = gi_ * gain[...]
    wide_g = cot[...].astype(F32) + inv * (gn - nrm * jnp.mean(gn * nrm, axis=1, keepdims=True))
    g[...] = wide_g.astype(BF)
    gcp = pltpu.make_async_copy(g, g_o, osem.at[4])
    gcp.start()
    for part in range(2):
        for n in range(8):
            h = part * 8 + n + (8 - 16 * part) * (1 - c)
            sqg[pl.ds(2 * h, 2)] = dot(qt[head(h), :], g[:, head(h)]).reshape(2, 64, HEAD).astype(BF)
        swaps.append(swap(sqg, oqg, (theirs, mine)[part], 2 + part))
    landed(oqg, mine, 2)
    tqg[...] = (sqg[mine].astype(F32) + oqg[mine].astype(F32)).astype(BF)
    scatter(tqg, qg1, 0, chip, 2)
    arrived(kv2, arsem.at[1])
    swaps.append(swap(kv2, kv2, mine, 4))
    gpart[1] = collect(0, cps0)
    cps1 = spread(1)

    def local_terms(h, carry):
        gh = g[:, head(h)]
        mix_a = jnp.where(tril, dot_nt(gh, vv[:, head(h)]), 0.0).astype(BF)
        gin[:, head(h)] = dot(mix_a, kv[:, head(h)])
        pk[:, head(h)] = dot_tn(mix_a, qv[:, head(h)])
        pv[:, head(h)] = dot_tn(mixb[h], gh)
        return carry

    lax.fori_loop(0, HEADS, local_terms, 0)
    arrived(qg1, arsem.at[2])

    def suffix(n, total):
        r = CHIPS - 1 - n
        qgs[r] = total.astype(BF)
        return total + qg1[r].astype(F32)

    lax.fori_loop(0, CHIPS, suffix, jnp.zeros((64, HEAD), F32))
    scatter(qgs, qg2, c * CHIPS, chip, 3)
    gpart[2] = collect(1, cps1)
    cps2 = spread(2)
    landed(okv, theirs, 1)
    landed(kv2, theirs, 4)
    second = c.astype(F32)

    def early_terms(h, carry):
        two = pl.ds(2 * h, 2)
        prior = (kv2[two].astype(F32) + second * okv[two].astype(F32)).reshape(HEAD, HEAD).astype(BF)
        gq[:, head(h)] = (scale * (gin[:, head(h)] + dot_nt(g[:, head(h)], prior))).astype(BF)
        return carry

    lax.fori_loop(0, HEADS, early_terms, 0)
    late = [pltpu.make_async_copy(gq, gq_o, osem.at[5])]
    late[0].start()
    gpart[3] = collect(2, cps2)
    cps3 = spread(3)
    arrived(qg2, arsem.at[3])
    swaps.append(swap(qg2, qg2, mine, 5))
    landed(oqg, theirs, 3)
    first = 1.0 - second
    for n in range(HEADS):
        if n == HEADS // 2:
            landed(qg2, theirs, 5)
        h = n + (1 - 2 * (n // 8)) * 8 * c
        at, two = head(h), pl.ds(2 * h, 2)
        later = (qg2[two].astype(F32) + first * oqg[two].astype(F32)).reshape(HEAD, HEAD).astype(BF)
        gk[:, at] = (scale * (pk[:, at] + dot_nt(vv[:, at], later))).astype(BF)
        gv[:, at] = (scale * (pv[:, at] + dot(kv[:, at], later))).astype(BF)
    gpart[4] = collect(3, cps3)
    for n, (a, b) in enumerate([(gk, gk_o), (gv, gv_o), (gpart.at[4], gain_o), (router, router_o)]):
        late.append(pltpu.make_async_copy(a, b, osem.at[6 + n]))
        late[-1].start()

    for kind in (0, 1):
        span = send.at[kind, pl.ds(1, DEV - 1)]
        pltpu.make_async_copy(span, span, fsem.at[kind]).wait()
    span = rsend.at[pl.ds(1, DEV - 1)]
    pltpu.make_async_copy(span, span, bsem).wait()
    for n, buf in enumerate((tkv, kvs, tqg, qgs)):
        arrived(buf, asem.at[n])
    for cp in swaps:
        cp.wait_send()
    for cp in store + [gcp] + late:
        cp.wait()


def call_mega(scale, operands):
    def vm(shape, dtype):
        return pltpu.VMEM(shape, dtype)

    state = (PLANE, 64, HEAD)
    results = [
        ((D, CAP), BF), ((CAP, D), BF), ((FF, CAP), BF), ((CAP, 2 * FF), BF), ((1, CAP), F32),
        ((TOK, D), BF), ((TOK, D), BF), ((TOK, D), BF), ((TOK, D), BF), ((1, D), F32),
    ]
    scratch = [
        vm((TOK, D), BF), vm((TOK, D), BF), vm((1, D), F32), vm((DEV, CAP), jnp.int32), vm((1, CAP), F32),
        vm((D, FF), BF), vm((D, FF), BF), vm((FF, D), BF),
        vm((TOK, D), BF), vm((TOK, D), BF), vm((TOK, D), BF),
        vm((TOK, D), F32), vm((2, 256, 1024), BF), vm((CAP, DEV), F32), vm((TOK, DEV), BF), vm((1024, 256), BF),
        vm((2, DEV, 16, 512), BF), vm((2, DEV, 16, 512), BF), vm((512, 1024), F32), vm((CAP, D), BF),
        vm((CAP, D), BF), vm((CAP, D), BF), vm((CAP, FF), F32), vm((CAP, FF), BF), vm((CAP, 2 * FF), BF),
        vm((D, CAP), BF), vm((FF, CAP), BF), vm((512, 1024), BF),
        vm((FF, D), BF), vm((FF, D), BF), vm((D, FF), BF),
        vm((DEV, 16, 512), BF), vm((DEV, 16, 512), BF),
        vm((TOK, D), F32), vm((TOK, D), BF),
        vm((D, TOK), BF),
    ] + [vm(state, BF)] * 6 + [vm((CHIPS, 64, HEAD), BF)] * 6 + [
        vm((HEADS, HEAD, HEAD), BF), vm((TOK, D), F32), vm((TOK, D), F32),
        vm((TOK, D), BF), vm((TOK, D), BF), vm((TOK, D), BF),
        vm((5, 1, D), F32), vm((4, 3, 1, D), F32), vm((1, CAP), F32),
    ]
    dma = pltpu.SemaphoreType.DMA
    sems = [
        dma((11,)), dma((10,)), dma((2,)), dma((2, 4)), dma, dma((4,)), dma((4,)), dma((4,)), dma((6,)), dma((6,)), dma((4, 3)), dma((4, 3)),
        pltpu.SemaphoreType.REGULAR,
    ]
    return pl.pallas_call(
        functools.partial(mega, scale),
        out_shape=[jax.ShapeDtypeStruct(a, b) for a, b in results],
        in_specs=[pl.BlockSpec(memory_space=pl.ANY)] * 11,
        out_specs=[pl.BlockSpec(memory_space=pl.ANY)] * len(results),
        scratch_shapes=scratch + sems,
        compiler_params=pltpu.CompilerParams(
            collective_id=0, has_side_effects=True, vmem_limit_bytes=63 * 1024 * 1024
        ),
        name="mega",
    )(*operands)


def finish(
    rowst_h, gout_h, hidt_h, dpre_h, router_h, g_h, gq_h, gk_h, gv_h, gain_h,
    gate_o, up_o, down_o, router_o, g_o, gq_o, gk_o, gv_o, gain_o,
    rowst, gout, hidt, dpre, router, g, gq, gk, gv, gain, gate, up, down, lsem, psem, wsem,
):
    ins = [(hidt_h, hidt), (gout_h, gout), (rowst_h, rowst), (dpre_h, dpre)]
    loads = [pltpu.make_async_copy(a, b, lsem.at[n]) for n, (a, b) in enumerate(ins)]
    through = [(g_h, g, g_o), (gq_h, gq, gq_o), (gk_h, gk, gk_o), (gv_h, gv, gv_o), (router_h, router, router_o),
               (gain_h, gain, gain_o)]
    take = [pltpu.make_async_copy(a, b, lsem.at[4 + n]) for n, (a, b, o) in enumerate(through)]
    give = [pltpu.make_async_copy(b, o, psem.at[n]) for n, (a, b, o) in enumerate(through)]
    for cp in loads + take:
        cp.start()
    writes = []

    def put(src, dst, rows):
        cp = pltpu.make_async_copy(src.at[rows], dst.at[rows], wsem.at[len(writes)])
        cp.start()
        writes.append(cp)

    loads[0].wait()
    loads[1].wait()
    for n in range(3):
        r = pl.ds(n * 256, 256)
        for m in range(2):
            col = pl.ds(m * 1024, 1024)
            down[r, col] = dot(hidt[r, :], gout[:, col]).astype(BF)
        put(down, down_o, r)
    loads[2].wait()
    loads[3].wait()
    for n in range(8):
        r = pl.ds(n * 256, 256)
        gate[r, :] = dot(rowst[r, :], dpre[:, 0:FF]).astype(BF)
        put(gate, gate_o, r)
        up[r, :] = dot(rowst[r, :], dpre[:, FF:]).astype(BF)
        put(up, up_o, r)
        if n < len(through):
            take[n].wait()
            give[n].start()
    for cp in give + writes:
        cp.wait()


def call_finish(operands):
    def vm(shape, dtype):
        return pltpu.VMEM(shape, dtype)

    small = [((1, CAP), F32), ((TOK, D), BF), ((TOK, D), BF), ((TOK, D), BF), ((TOK, D), BF), ((1, D), F32)]
    weights = [((D, FF), BF), ((D, FF), BF), ((FF, D), BF)]
    dma = pltpu.SemaphoreType.DMA
    return pl.pallas_call(
        finish,
        out_shape=[jax.ShapeDtypeStruct(a, b) for a, b in weights + small],
        in_specs=[pl.BlockSpec(memory_space=pl.ANY)] * 10,
        out_specs=[pl.BlockSpec(memory_space=pl.ANY)] * 9,
        scratch_shapes=[vm((D, CAP), BF), vm((CAP, D), BF), vm((FF, CAP), BF), vm((CAP, 2 * FF), BF)]
        + [vm(a, b) for a, b in small + weights]
        + [dma((10,)), dma((6,)), dma((19,))],
        compiler_params=pltpu.CompilerParams(vmem_limit_bytes=63 * 1024 * 1024),
        name="finish",
    )(*operands)


def body(stream, cotangent, norm_gain, queries, key_vectors, value_vectors, expert_index, router_gates,
         gate_proj, up_proj, down_proj):
    scale = 1.0 / math.sqrt(HEAD * TOK * PLANE)
    results = call_mega(scale, (
        stream, cotangent, norm_gain[None, :], expert_index, router_gates, gate_proj[0], up_proj[0], down_proj[0],
        queries, key_vectors, value_vectors,
    ))
    gate, up, down, router, g, gq, gk, gv, gain = call_finish(results)
    return (g, gq, gk, gv, gate[None], up[None], down[None], router, gain[0])


def solution(mesh):
    both = ("grp", "seq")
    r2, r3 = P(both, None), P(both, None, None)
    return jax.shard_map(
        body,
        mesh=mesh,
        in_specs=(r2, r2, P(), r2, r2, r2, P(), r2, r3, r3, r3),
        out_specs=(r2, r2, r2, r2, r3, r3, r3, r2, P()),
        check_vma=False,
    )
```

```python
import functools
import math

import jax
import jax.numpy as jnp
from jax import lax
from jax.experimental import pallas as pl
from jax.experimental.pallas import tpu as pltpu
from jax.sharding import PartitionSpec as P

D = 2048
FF = 768
HEADS = 16
HEAD = 128
CAP = 256
TOK = 128
DEV = 128
PLANE = 32
CHIPS = 16
CHIP_MULT = 7
SLOTS = 4
EPS = 1e-06
MULT = 91
MULT_INV = 83
PLANE_MULT = 13
MESH = pl.DeviceIdType.MESH
BF = jnp.bfloat16
F32 = jnp.float32


def dot(a, b):
    return lax.dot_general(a, b, (((1,), (0,)), ((), ())), preferred_element_type=F32)


def dot_nt(a, b):
    return lax.dot_general(a, b, (((1,), (1,)), ((), ())), preferred_element_type=F32)


def dot_tn(a, b):
    return lax.dot_general(a, b, (((0,), (0,)), ((), ())), preferred_element_type=F32)


def rem(a, n):
    return lax.rem(a, jnp.int32(n))


def div(a, n):
    return lax.div(a, jnp.int32(n))


def offsets(i):
    k = rem(i * MULT, DEV)
    return div(k, 32), rem(div(k, 8), 4), rem(div(k, 2), 4), rem(k, 2)


def index_of(z, x, y, c):
    return rem(z, 4), rem(x, 4) * 8 + rem(y, 4) * 2 + rem(c, 2)


def mega(
    scale,
    stream_h, cot_h, gain_h, index_h, gates_h, wg_h, wu_h, wd_h, q_h, k_h, v_h,
    rows_o, gout_o, hid_o, dpre_o, router_o, g_o, gq_o, gk_o, gv_o, gain_o,
    stream, cot, gain, index, gates, wg, wu, wd, qv, kv, vv,
    normed, xin, tindex, code, p8, send, recv, acc, rows, dy, gout, ghid, hid, dpre, rowst, hidt, stacked,
    wgt, wut, wdt, rsend, rrecv,
    gin, g, qt, skv, sqg, okv, oqg, kv2, qg2, tkv, kv1, kvs, tqg, qg1, qgs, mixb, pk, pv, gq, gk, gv, gpart, gland, router,
    lsem, osem, fsem, frsem, bsem, brsem, asem, arsem, wsem, wrsem, gsem, grsem, zsem,
):
    z = lax.axis_index("grp")
    s = lax.axis_index("seq")
    x, y, c = div(s, 8), rem(div(s, 2), 4), rem(s, 2)

    def dev(z2, s2):
        return {"grp": z2, "seq": s2}

    def out_to(i):
        dz, dx, dy, dc = offsets(i)
        return dev(*index_of(z + dz, x + dx, y + dy, c + dc))

    def back_to(i):
        dz, dx, dy, dc = offsets(i)
        return dev(*index_of(z + 4 - dz, x + 4 - dx, y + 4 - dy, c + dc))

    def plane_to(j):
        k = rem(j * PLANE_MULT, PLANE)
        return index_of(z, x + div(k, 8), y + rem(div(k, 2), 4), c + rem(k, 2))[1]

    bar = pltpu.get_barrier_semaphore()

    def greet(j, carry):
        pl.semaphore_signal(bar, inc=1, device_id=dev(z, plane_to(j)), device_id_type=MESH)
        return carry

    lax.fori_loop(1, PLANE, greet, 0)
    for d in (1, 2, 3):
        pl.semaphore_signal(bar, inc=1, device_id=dev(rem(z + d, 4), s), device_id_type=MESH)

    loads = [
        (index_h, index), (stream_h, stream), (cot_h, cot), (gain_h, gain),
        (gates_h, gates), (q_h, qv), (k_h, kv), (v_h, vv), (wg_h, wg), (wu_h, wu), (wd_h, wd),
    ]
    load = [pltpu.make_async_copy(a, b, lsem.at[n]) for n, (a, b) in enumerate(loads)]
    for cp in load:
        cp.start()

    load[0].wait()
    here = z * PLANE + s
    tindex[...] = (index[...] - here * TOK).astype(F32).T
    token = lax.broadcasted_iota(jnp.int32, (TOK, DEV), 0).astype(F32)

    def match(n, found):
        eight = tindex[pl.ds(pl.multiple_of(n * 8, 8), 8), :]
        for r in range(8):
            found = jnp.where(eight[r:r + 1, :] == token, 1.0, found)
        return found

    found = lax.fori_loop(0, CAP // 8, match, jnp.zeros((TOK, DEV), F32), unroll=2)
    earlier = lax.broadcasted_iota(jnp.int32, (TOK, TOK), 0) > lax.broadcasted_iota(jnp.int32, (TOK, TOK), 1)
    before = dot(jnp.where(earlier, 1.0, 0.0).astype(BF), found.astype(BF))
    code[...] = (found * (before + 1.0)).astype(BF)

    pl.semaphore_wait(bar, PLANE - 1 + 3)
    for d in (1, 2, 3):
        pl.semaphore_signal(zsem, inc=1, device_id=dev(rem(z + d, 4), s), device_id_type=MESH)

    def build(gi, carry):
        r = lax.broadcasted_iota(jnp.int32, (256, 128), 0) + gi * 256
        lane = lax.broadcasted_iota(jnp.int32, (256, 128), 1)
        k = ((r >> 3) * MULT) & (DEV - 1)
        e = ((z + (k >> 5)) & 3) * 32 + ((x + (k >> 3)) & 3) * 8 + ((y + (k >> 1)) & 3) * 2 + ((c + k) & 1)
        pick = jnp.where(e == lane, 1.0, 0.0).astype(BF)
        rep = dot_nt(pick, code[...])
        want = ((r & 3) + 1).astype(F32)
        hit = jnp.where(rep == want, 1.0, 0.0)
        half = (r >> 2) & 1
        row0 = pl.multiple_of(gi * 256, 256)
        p8[pl.ds(row0, 256), 0:128] = jnp.where(half == 0, hit, 0.0).astype(BF)
        p8[pl.ds(row0, 256), 128:256] = jnp.where(half == 1, hit, 0.0).astype(BF)
        return carry

    lax.fori_loop(0, 4, build, 0, unroll=True)

    def fold(o):
        o = o.reshape(32, 8, 1024)
        return jnp.concatenate([o[:, :, 0:512], o[:, :, 512:1024]], axis=1).astype(BF)

    def fill(kind):
        def one(gi, carry):
            row0 = pl.multiple_of(gi * 256, 256)
            send[kind, pl.ds(gi * 32, 32)] = fold(dot(p8[pl.ds(row0, 256), :], xin[kind]))
            return carry

        lax.fori_loop(0, 4, one, 0)

    def push(kind):
        def one(i, carry):
            pltpu.make_async_remote_copy(
                send.at[kind, i], recv.at[kind, i], fsem.at[kind], frsem.at[kind, div(i, 32)],
                device_id=out_to(i), device_id_type=MESH,
            ).start()
            return carry

        lax.fori_loop(1, DEV, one, 0)
        recv[kind, 0] = send[kind, 0]

    load[2].wait()
    xin[0, 0:TOK, :] = cot[:, 0:1024]
    xin[0, TOK:, :] = cot[:, 1024:]
    fill(0)
    pl.semaphore_wait(zsem, 3)
    push(0)

    load[1].wait()
    load[3].wait()
    wide = stream[...].astype(F32)
    inv = lax.rsqrt(jnp.mean(wide * wide, axis=1, keepdims=True) + EPS)
    nrm = wide * inv
    normed[...] = nrm
    xin[1, 0:TOK, :] = (nrm * gain[...])[:, 0:1024].astype(BF)
    xin[1, TOK:, :] = (nrm * gain[...])[:, 1024:].astype(BF)
    fill(1)
    push(1)

    for n in (4, 5, 6, 7):
        load[n].wait()
    tril = lax.broadcasted_iota(jnp.int32, (TOK, TOK), 0) >= lax.broadcasted_iota(jnp.int32, (TOK, TOK), 1)

    def head(h):
        return pl.ds(pl.multiple_of(h * HEAD, HEAD), HEAD)

    def local_kv(h, carry):
        kh = kv[:, head(h)]
        skv[pl.ds(2 * h, 2)] = dot_tn(kh, vv[:, head(h)]).reshape(2, 64, HEAD).astype(BF)
        qt[head(h), :] = qv[:, head(h)].T
        mixb[h] = jnp.where(tril, dot_nt(qv[:, head(h)], kh), 0.0).astype(BF)
        return carry

    lax.fori_loop(0, HEADS, local_kv, 0, unroll=4)

    chip = x * 4 + y
    mine = pl.ds(c * CHIPS, CHIPS)
    theirs = pl.ds((1 - c) * CHIPS, CHIPS)

    def swap(src, dst, part, n):
        cp = pltpu.make_async_remote_copy(
            src.at[part], dst.at[part], wsem.at[n], wrsem.at[n], device_id=dev(z, s + 1 - 2 * c), device_id_type=MESH
        )
        cp.start()
        return cp

    def landed(dst, part, n):
        span = dst.at[part]
        pltpu.make_async_copy(span, span, wrsem.at[n]).wait()

    def scatter(src, dst, base, at, n):
        def one(j, carry):
            k = rem(j * CHIP_MULT, CHIPS)
            x2, y2 = rem(x + div(k, 4), 4), rem(y + rem(k, 4), 4)
            pltpu.make_async_remote_copy(
                src.at[x2 * 4 + y2], dst.at[base + at], asem.at[n], arsem.at[n],
                device_id=dev(z, x2 * 8 + y2 * 2 + c), device_id_type=MESH,
            ).start()
            return carry

        lax.fori_loop(1, CHIPS, one, 0)
        dst[base + at] = src[at]

    reach = sorted(
        [(dx, dy) for dx in range(4) for dy in range(4) if dx + dy],
        key=lambda o: (-min(o[0], 4 - o[0]) - min(o[1], 4 - o[1]), o[0] + 2 * o[1]),
    )

    def scatter_far(src, dst, base, at, n):
        for dx, dy in reach:
            x2, y2 = rem(x + dx, 4), rem(y + dy, 4)
            pltpu.make_async_remote_copy(
                src.at[x2 * 4 + y2], dst.at[base + at], asem.at[n], arsem.at[n],
                device_id=dev(z, x2 * 8 + y2 * 2 + c), device_id_type=MESH,
            ).start()
        dst[base + at] = src[at]

    def arrived(dst, sem):
        span = dst.at[pl.ds(0, CHIPS - 1)]
        pltpu.make_async_copy(span, span, sem).wait()

    swaps = [swap(skv, okv, theirs, 0), swap(skv, okv, mine, 1)]

    own_row = index[pl.ds(here, 1), :]
    own_col = jnp.broadcast_to(own_row.astype(F32), (8, CAP)).T[:, 0:1].astype(jnp.int32)
    wide_row = jnp.broadcast_to(own_row, (CAP, CAP))
    wide_col = jnp.broadcast_to(own_col, (CAP, CAP))
    mate = (wide_row >> 7) == (wide_col >> 7)
    slot_col = jnp.sum(jnp.where(mate & (wide_row < wide_col), 1.0, 0.0), axis=1, keepdims=True)
    slot_row = jnp.sum(jnp.where(mate & (wide_col < wide_row), 1.0, 0.0), axis=0, keepdims=True)

    def place(own, slot):
        src = own >> 7
        k = (
            ((z - (src >> 5)) & 3) * 32 + ((x - (src >> 3)) & 3) * 8 + ((y - (src >> 1)) & 3) * 2 + ((c - src) & 1)
        )
        return ((k * MULT_INV) & (DEV - 1)) * 8 + slot.astype(jnp.int32)

    at_col = place(own_col, slot_col)
    at_row = place(own_row, slot_row)
    tcol = jnp.concatenate([at_col, at_col + 4], axis=0)
    trow = jnp.concatenate([at_row, at_row + 4], axis=1)
    gate_col = jnp.broadcast_to(gates[...], (8, CAP)).T[:, 0:1]

    for n in (8, 9, 10):
        load[n].wait()

    def turn_weights(n, carry):
        c0 = pl.multiple_of(n * 256, 256)
        wgt[:, pl.ds(c0, 256)] = wg[pl.ds(c0, 256), :].T
        wut[:, pl.ds(c0, 256)] = wu[pl.ds(c0, 256), :].T
        wdt[pl.ds(c0, 256), :] = wd[:, pl.ds(c0, 256)].T
        return carry

    lax.fori_loop(0, 8, turn_weights, 0)
    landed(okv, mine, 0)
    tkv[...] = (skv[mine].astype(F32) + okv[mine].astype(F32)).astype(BF)
    scatter(tkv, kv1, 0, chip, 0)

    def settle(kind, dst):
        for gi in range(4):
            first = 1 if gi == 0 else 0
            span = recv.at[kind, pl.ds(gi * 32 + first, 32 - first)]
            pltpu.make_async_copy(span, span, frsem.at[kind, gi]).wait()
            lane = lax.broadcasted_iota(jnp.int32, (512, 256), 1) + gi * 256
            put = jnp.where(lane == tcol, 1.0, 0.0).astype(BF)
            for half in range(2):
                f = recv[kind, pl.ds(gi * 32, 32)].astype(F32).reshape(32, 2, 8, 512)[:, half]
                part = dot(put, f.reshape(256, 512).astype(BF))
                at = slice(half * 512, (half + 1) * 512)
                if gi == 0:
                    acc[:, at] = part
                elif gi < 3:
                    acc[:, at] += part
                else:
                    part = (acc[:, at] + part).astype(BF)
                    dst[:, half * 512:(half + 1) * 512] = part[0:CAP]
                    dst[:, 1024 + half * 512:1024 + (half + 1) * 512] = part[CAP:]

    settle(0, dy)
    gout[...] = (gate_col * dy[...].astype(F32)).astype(BF)
    ghid[...] = dot(gout[...], wdt[...])
    settle(1, rows)

    def front(n, carry):
        c0 = pl.multiple_of(n * 256, 256)
        gp = dot(rows[...], wg[:, pl.ds(c0, 256)])
        up = dot(rows[...], wu[:, pl.ds(c0, 256)])
        gh = ghid[:, pl.ds(c0, 256)]
        sg = jax.nn.sigmoid(gp)
        silu = gp * sg
        hid[:, pl.ds(c0, 256)] = (silu * up).astype(BF)
        dpre[:, pl.ds(c0, 256)] = (gh * up * (sg * (1.0 + gp * (1.0 - sg)))).astype(BF)
        dpre[:, pl.ds(pl.multiple_of(c0 + FF, 256), 256)] = (gh * silu).astype(BF)
        return carry

    lax.fori_loop(0, 3, front, 0, unroll=True)

    def back(n, carry):
        r0 = pl.multiple_of(n * 256, 256)
        gr = dot(dpre[:, 0:FF], wgt[:, pl.ds(r0, 256)]) + dot(dpre[:, FF:], wut[:, pl.ds(r0, 256)])
        h0 = pl.multiple_of(div(n, 4) * 256, 256)
        c0 = pl.multiple_of(rem(n, 4) * 256, 256)
        stacked[pl.ds(h0, 256), pl.ds(c0, 256)] = gr.astype(BF)
        return carry

    lax.fori_loop(0, 8, back, 0, unroll=4)

    def refill(gi, carry):
        r = lax.broadcasted_iota(jnp.int32, (256, 512), 0) + gi * 256
        put = jnp.where(r == trow, 1.0, 0.0).astype(BF)
        rsend[pl.ds(gi * 32, 32)] = fold(dot(put, stacked[...]))
        return carry

    def ret(i, carry):
        pltpu.make_async_remote_copy(
            rsend.at[i], rrecv.at[i], bsem, brsem.at[div(i, 32)], device_id=back_to(i), device_id_type=MESH
        ).start()
        return carry

    lax.fori_loop(0, 2, refill, 0)
    lax.fori_loop(1, 32, ret, 0)
    lax.fori_loop(2, 3, refill, 0)
    lax.fori_loop(32, 64, ret, 0)
    lax.fori_loop(3, 4, refill, 0)
    lax.fori_loop(64, 128, ret, 0)
    rrecv[0] = rsend[0]

    def turn(n, carry):
        c0 = pl.multiple_of(n * 256, 256)
        rowst[pl.ds(c0, 256), :] = rows[:, pl.ds(c0, 256)].T
        return carry

    lax.fori_loop(0, 8, turn, 0)
    for n in range(3):
        hidt[n * 256:(n + 1) * 256, :] = hid[:, n * 256:(n + 1) * 256].T
    outs = [(rowst, rows_o), (gout, gout_o), (hidt, hid_o), (dpre, dpre_o)]
    store = [pltpu.make_async_copy(a, b, osem.at[n]) for n, (a, b) in enumerate(outs)]
    for cp in store:
        cp.start()

    def route(n, total):
        c0 = pl.multiple_of(n * 256, 256)
        eo = dot(hid[...], wd[:, pl.ds(c0, 256)])
        return total + jnp.sum(dy[:, pl.ds(c0, 256)].astype(F32) * eo, axis=1, keepdims=True)

    router_col = lax.fori_loop(0, 8, route, jnp.zeros((CAP, 1), F32))
    router[...] = jnp.broadcast_to(router_col, (CAP, 128)).T[0:1, :]

    arrived(kv1, arsem.at[0])

    def prefix(r, total):
        kvs[r] = total.astype(BF)
        return total + kv1[r].astype(F32)

    lax.fori_loop(0, CHIPS, prefix, jnp.zeros((64, HEAD), F32), unroll=True)
    scatter(kvs, kv2, c * CHIPS, chip, 1)

    for gi in range(4):
        first = 1 if gi == 0 else 0
        span = rrecv.at[pl.ds(gi * 32 + first, 32 - first)]
        pltpu.make_async_copy(span, span, brsem.at[gi]).wait()
        for half in range(2):
            f = rrecv[pl.ds(gi * 32, 32)].astype(F32).reshape(32, 2, 8, 512)[:, half]
            f = f.reshape(256, 512).astype(BF)
            part = dot_tn(p8[gi * 256:(gi + 1) * 256, :], f)
            for hh in range(2):
                c0 = hh * 1024 + half * 512
                piece = part[hh * TOK:(hh + 1) * TOK, :]
                if gi == 0:
                    gin[:, c0:c0 + 512] = piece
                else:
                    gin[:, c0:c0 + 512] += piece

    gi_ = gin[...]
    nrm = normed[...]

    def spread(stage):
        if stage == 0:
            to = [dev(z, s + 1 - 2 * c)]
        elif stage == 1:
            to = [dev(z, x * 8 + rem(y + d, 4) * 2 + c) for d in (1, 2, 3)]
        elif stage == 2:
            to = [dev(z, rem(x + d, 4) * 8 + y * 2 + c) for d in (1, 2, 3)]
        else:
            to = [dev(rem(z + d, 4), s) for d in (1, 2, 3)]
        cps = [
            pltpu.make_async_remote_copy(
                gpart.at[stage], gland.at[stage, d], gsem.at[stage, d], grsem.at[stage, d],
                device_id=t, device_id_type=MESH,
            )
            for d, t in enumerate(to)
        ]
        for cp in cps:
            cp.start()
        return cps

    def collect(stage, cps):
        for cp in cps:
            cp.wait()
        total = gpart[stage]
        for d in range(len(cps)):
            total = total + gland[stage, d]
        return total

    gpart[0] = jnp.sum(gi_ * nrm, axis=0, keepdims=True)
    cps0 = spread(0)

    gn = gi_ * gain[...]
    wide_g = cot[...].astype(F32) + inv * (gn - nrm * jnp.mean(gn * nrm, axis=1, keepdims=True))
    g[...] = wide_g.astype(BF)
    gcp = pltpu.make_async_copy(g, g_o, osem.at[4])
    gcp.start()
    for part in range(2):
        for n in range(8):
            h = part * 8 + n + (8 - 16 * part) * (1 - c)
            sqg[pl.ds(2 * h, 2)] = dot(qt[head(h), :], g[:, head(h)]).reshape(2, 64, HEAD).astype(BF)
        swaps.append(swap(sqg, oqg, (theirs, mine)[part], 2 + part))
    landed(oqg, mine, 2)
    tqg[...] = (sqg[mine].astype(F32) + oqg[mine].astype(F32)).astype(BF)
    scatter_far(tqg, qg1, 0, chip, 2)
    arrived(kv2, arsem.at[1])
    swaps.append(swap(kv2, kv2, mine, 4))
    gpart[1] = collect(0, cps0)
    cps1 = spread(1)

    def local_terms(h, carry):
        gh = g[:, head(h)]
        mix_a = jnp.where(tril, dot_nt(gh, vv[:, head(h)]), 0.0).astype(BF)
        gin[:, head(h)] = dot(mix_a, kv[:, head(h)])
        pk[:, head(h)] = dot_tn(mix_a, qv[:, head(h)])
        pv[:, head(h)] = dot_tn(mixb[h], gh)
        return carry

    lax.fori_loop(0, HEADS, local_terms, 0, unroll=4)
    arrived(qg1, arsem.at[2])

    def suffix(n, total):
        r = CHIPS - 1 - n
        qgs[r] = total.astype(BF)
        return total + qg1[r].astype(F32)

    lax.fori_loop(0, CHIPS, suffix, jnp.zeros((64, HEAD), F32), unroll=True)
    scatter_far(qgs, qg2, c * CHIPS, chip, 3)
    gpart[2] = collect(1, cps1)
    cps2 = spread(2)
    landed(okv, theirs, 1)
    landed(kv2, theirs, 4)
    second = c.astype(F32)

    def early_terms(h, carry):
        two = pl.ds(2 * h, 2)
        prior = (kv2[two].astype(F32) + second * okv[two].astype(F32)).reshape(HEAD, HEAD).astype(BF)
        gq[:, head(h)] = (scale * (gin[:, head(h)] + dot_nt(g[:, head(h)], prior))).astype(BF)
        return carry

    lax.fori_loop(0, HEADS, early_terms, 0, unroll=4)
    late = [pltpu.make_async_copy(gq, gq_o, osem.at[5])]
    late[0].start()
    gpart[3] = collect(2, cps2)
    cps3 = spread(3)
    arrived(qg2, arsem.at[3])
    swaps.append(swap(qg2, qg2, mine, 5))
    landed(oqg, theirs, 3)
    first = 1.0 - second
    for n in range(HEADS):
        if n == HEADS // 2:
            landed(qg2, theirs, 5)
        h = n + (1 - 2 * (n // 8)) * 8 * c
        at, two = head(h), pl.ds(2 * h, 2)
        later = (qg2[two].astype(F32) + first * oqg[two].astype(F32)).reshape(HEAD, HEAD).astype(BF)
        gk[:, at] = (scale * (pk[:, at] + dot_nt(vv[:, at], later))).astype(BF)
        gv[:, at] = (scale * (pv[:, at] + dot(kv[:, at], later))).astype(BF)
    gpart[4] = collect(3, cps3)
    for n, (a, b) in enumerate([(gk, gk_o), (gv, gv_o), (gpart.at[4], gain_o), (router, router_o)]):
        late.append(pltpu.make_async_copy(a, b, osem.at[6 + n]))
        late[-1].start()

    for kind in (0, 1):
        span = send.at[kind, pl.ds(1, DEV - 1)]
        pltpu.make_async_copy(span, span, fsem.at[kind]).wait()
    span = rsend.at[pl.ds(1, DEV - 1)]
    pltpu.make_async_copy(span, span, bsem).wait()
    for n, buf in enumerate((tkv, kvs, tqg, qgs)):
        arrived(buf, asem.at[n])
    for cp in swaps:
        cp.wait_send()
    for cp in store + [gcp] + late:
        cp.wait()


def call_mega(scale, operands):
    def vm(shape, dtype):
        return pltpu.VMEM(shape, dtype)

    state = (PLANE, 64, HEAD)
    results = [
        ((D, CAP), BF), ((CAP, D), BF), ((FF, CAP), BF), ((CAP, 2 * FF), BF), ((1, CAP), F32),
        ((TOK, D), BF), ((TOK, D), BF), ((TOK, D), BF), ((TOK, D), BF), ((1, D), F32),
    ]
    scratch = [
        vm((TOK, D), BF), vm((TOK, D), BF), vm((1, D), F32), vm((DEV, CAP), jnp.int32), vm((1, CAP), F32),
        vm((D, FF), BF), vm((D, FF), BF), vm((FF, D), BF),
        vm((TOK, D), BF), vm((TOK, D), BF), vm((TOK, D), BF),
        vm((TOK, D), F32), vm((2, 256, 1024), BF), vm((CAP, DEV), F32), vm((TOK, DEV), BF), vm((1024, 256), BF),
        vm((2, DEV, 16, 512), BF), vm((2, DEV, 16, 512), BF), vm((512, 1024), F32), vm((CAP, D), BF),
        vm((CAP, D), BF), vm((CAP, D), BF), vm((CAP, FF), F32), vm((CAP, FF), BF), vm((CAP, 2 * FF), BF),
        vm((D, CAP), BF), vm((FF, CAP), BF), vm((512, 1024), BF),
        vm((FF, D), BF), vm((FF, D), BF), vm((D, FF), BF),
        vm((DEV, 16, 512), BF), vm((DEV, 16, 512), BF),
        vm((TOK, D), F32), vm((TOK, D), BF),
        vm((D, TOK), BF),
    ] + [vm(state, BF)] * 6 + [vm((CHIPS, 64, HEAD), BF)] * 6 + [
        vm((HEADS, HEAD, HEAD), BF), vm((TOK, D), F32), vm((TOK, D), F32),
        vm((TOK, D), BF), vm((TOK, D), BF), vm((TOK, D), BF),
        vm((5, 1, D), F32), vm((4, 3, 1, D), F32), vm((1, CAP), F32),
    ]
    dma = pltpu.SemaphoreType.DMA
    sems = [
        dma((11,)), dma((10,)), dma((2,)), dma((2, 4)), dma, dma((4,)), dma((4,)), dma((4,)), dma((6,)), dma((6,)), dma((4, 3)), dma((4, 3)),
        pltpu.SemaphoreType.REGULAR,
    ]
    return pl.pallas_call(
        functools.partial(mega, scale),
        out_shape=[jax.ShapeDtypeStruct(a, b) for a, b in results],
        in_specs=[pl.BlockSpec(memory_space=pl.ANY)] * 11,
        out_specs=[pl.BlockSpec(memory_space=pl.ANY)] * len(results),
        scratch_shapes=scratch + sems,
        compiler_params=pltpu.CompilerParams(
            collective_id=0, has_side_effects=True, vmem_limit_bytes=63 * 1024 * 1024
        ),
        name="mega",
    )(*operands)


def finish(
    rowst_h, gout_h, hidt_h, dpre_h, router_h, g_h, gq_h, gk_h, gv_h, gain_h,
    gate_o, up_o, down_o, router_o, g_o, gq_o, gk_o, gv_o, gain_o,
    rowst, gout, hidt, dpre, router, g, gq, gk, gv, gain, gate, up, down, lsem, psem, wsem,
):
    ins = [(hidt_h, hidt), (gout_h, gout), (rowst_h, rowst), (dpre_h, dpre)]
    loads = [pltpu.make_async_copy(a, b, lsem.at[n]) for n, (a, b) in enumerate(ins)]
    through = [(g_h, g, g_o), (gq_h, gq, gq_o), (gk_h, gk, gk_o), (gv_h, gv, gv_o), (router_h, router, router_o),
               (gain_h, gain, gain_o)]
    take = [pltpu.make_async_copy(a, b, lsem.at[4 + n]) for n, (a, b, o) in enumerate(through)]
    give = [pltpu.make_async_copy(b, o, psem.at[n]) for n, (a, b, o) in enumerate(through)]
    for cp in loads + take:
        cp.start()
    writes = []

    def put(src, dst, rows):
        cp = pltpu.make_async_copy(src.at[rows], dst.at[rows], wsem.at[len(writes)])
        cp.start()
        writes.append(cp)

    loads[0].wait()
    loads[1].wait()
    for n in range(3):
        r = pl.ds(n * 256, 256)
        for m in range(2):
            col = pl.ds(m * 1024, 1024)
            down[r, col] = dot(hidt[r, :], gout[:, col]).astype(BF)
        put(down, down_o, r)
    loads[2].wait()
    loads[3].wait()
    for n in range(8):
        r = pl.ds(n * 256, 256)
        gate[r, :] = dot(rowst[r, :], dpre[:, 0:FF]).astype(BF)
        put(gate, gate_o, r)
        up[r, :] = dot(rowst[r, :], dpre[:, FF:]).astype(BF)
        put(up, up_o, r)
        if n < len(through):
            take[n].wait()
            give[n].start()
    for cp in give + writes:
        cp.wait()


def call_finish(operands):
    def vm(shape, dtype):
        return pltpu.VMEM(shape, dtype)

    small = [((1, CAP), F32), ((TOK, D), BF), ((TOK, D), BF), ((TOK, D), BF), ((TOK, D), BF), ((1, D), F32)]
    weights = [((D, FF), BF), ((D, FF), BF), ((FF, D), BF)]
    dma = pltpu.SemaphoreType.DMA
    return pl.pallas_call(
        finish,
        out_shape=[jax.ShapeDtypeStruct(a, b) for a, b in weights + small],
        in_specs=[pl.BlockSpec(memory_space=pl.ANY)] * 10,
        out_specs=[pl.BlockSpec(memory_space=pl.ANY)] * 9,
        scratch_shapes=[vm((D, CAP), BF), vm((CAP, D), BF), vm((FF, CAP), BF), vm((CAP, 2 * FF), BF)]
        + [vm(a, b) for a, b in small + weights]
        + [dma((10,)), dma((6,)), dma((19,))],
        compiler_params=pltpu.CompilerParams(vmem_limit_bytes=63 * 1024 * 1024),
        name="finish",
    )(*operands)


def body(stream, cotangent, norm_gain, queries, key_vectors, value_vectors, expert_index, router_gates,
         gate_proj, up_proj, down_proj):
    scale = 1.0 / math.sqrt(HEAD * TOK * PLANE)
    results = call_mega(scale, (
        stream, cotangent, norm_gain[None, :], expert_index, router_gates, gate_proj[0], up_proj[0], down_proj[0],
        queries, key_vectors, value_vectors,
    ))
    gate, up, down, router, g, gq, gk, gv, gain = call_finish(results)
    return (g, gq, gk, gv, gate[None], up[None], down[None], router, gain[0])


def solution(mesh):
    both = ("grp", "seq")
    r2, r3 = P(both, None), P(both, None, None)
    return jax.shard_map(
        body,
        mesh=mesh,
        in_specs=(r2, r2, P(), r2, r2, r2, P(), r2, r3, r3, r3),
        out_specs=(r2, r2, r2, r2, r3, r3, r3, r2, P()),
        check_vma=False,
    )
```

```python
import functools
import math

import jax
import jax.numpy as jnp
from jax import lax
from jax.experimental import pallas as pl
from jax.experimental.pallas import tpu as pltpu
from jax.sharding import PartitionSpec as P

D = 2048
FF = 768
HEADS = 16
HEAD = 128
CAP = 256
TOK = 128
DEV = 128
PLANE = 32
CHIPS = 16
CHIP_MULT = 7
SLOTS = 4
EPS = 1e-06
MULT = 91
MULT_INV = 83
PLANE_MULT = 13
MESH = pl.DeviceIdType.MESH
BF = jnp.bfloat16
F32 = jnp.float32


def dot(a, b):
    return lax.dot_general(a, b, (((1,), (0,)), ((), ())), preferred_element_type=F32)


def dot_nt(a, b):
    return lax.dot_general(a, b, (((1,), (1,)), ((), ())), preferred_element_type=F32)


def dot_tn(a, b):
    return lax.dot_general(a, b, (((0,), (0,)), ((), ())), preferred_element_type=F32)


def rem(a, n):
    return lax.rem(a, jnp.int32(n))


def div(a, n):
    return lax.div(a, jnp.int32(n))


def offsets(i):
    k = rem(i * MULT, DEV)
    return div(k, 32), rem(div(k, 8), 4), rem(div(k, 2), 4), rem(k, 2)


def index_of(z, x, y, c):
    return rem(z, 4), rem(x, 4) * 8 + rem(y, 4) * 2 + rem(c, 2)


def mega(
    scale,
    stream_h, cot_h, gain_h, index_h, gates_h, wg_h, wu_h, wd_h, q_h, k_h, v_h,
    rows_o, gout_o, hid_o, dpre_o, router_o, g_o, gq_o, gk_o, gv_o, gain_o,
    stream, cot, gain, index, gates, wg, wu, wd, qv, kv, vv,
    normed, xin, tindex, code, p8, p8t, send, recv, acc, rows, dy, gout, ghid, hid, dpre, rowst, hidt, stacked,
    wgt, wut, wdt, rsend, rrecv,
    gin, g, qt, skv, sqg, okv, oqg, kv2, qg2, tkv, kv1, kvs, tqg, qg1, qgs, mixb, pk, pv, gq, gk, gv, gpart, gland, router,
    lsem, osem, fsem, frsem, bsem, brsem, asem, arsem, wsem, wrsem, gsem, grsem, zsem,
):
    z = lax.axis_index("grp")
    s = lax.axis_index("seq")
    x, y, c = div(s, 8), rem(div(s, 2), 4), rem(s, 2)

    def dev(z2, s2):
        return {"grp": z2, "seq": s2}

    def out_to(i):
        dz, dx, dy, dc = offsets(i)
        return dev(*index_of(z + dz, x + dx, y + dy, c + dc))

    def back_to(i):
        dz, dx, dy, dc = offsets(i)
        return dev(*index_of(z + 4 - dz, x + 4 - dx, y + 4 - dy, c + dc))

    def plane_to(j):
        k = rem(j * PLANE_MULT, PLANE)
        return index_of(z, x + div(k, 8), y + rem(div(k, 2), 4), c + rem(k, 2))[1]

    bar = pltpu.get_barrier_semaphore()

    def greet(j, carry):
        pl.semaphore_signal(bar, inc=1, device_id=dev(z, plane_to(j)), device_id_type=MESH)
        return carry

    lax.fori_loop(1, PLANE, greet, 0)
    for d in (1, 2, 3):
        pl.semaphore_signal(bar, inc=1, device_id=dev(rem(z + d, 4), s), device_id_type=MESH)

    loads = [
        (index_h, index), (stream_h, stream), (cot_h, cot), (gain_h, gain),
        (gates_h, gates), (q_h, qv), (k_h, kv), (v_h, vv), (wg_h, wg), (wu_h, wu), (wd_h, wd),
    ]
    load = [pltpu.make_async_copy(a, b, lsem.at[n]) for n, (a, b) in enumerate(loads)]
    for cp in load:
        cp.start()

    load[0].wait()
    here = z * PLANE + s
    tindex[...] = (index[...] - here * TOK).astype(F32).T
    token = lax.broadcasted_iota(jnp.int32, (TOK, DEV), 0).astype(F32)

    def match(n, found):
        eight = tindex[pl.ds(pl.multiple_of(n * 8, 8), 8), :]
        for r in range(8):
            found = jnp.where(eight[r:r + 1, :] == token, 1.0, found)
        return found

    found = lax.fori_loop(0, CAP // 8, match, jnp.zeros((TOK, DEV), F32), unroll=2)
    earlier = lax.broadcasted_iota(jnp.int32, (TOK, TOK), 0) > lax.broadcasted_iota(jnp.int32, (TOK, TOK), 1)
    before = dot(jnp.where(earlier, 1.0, 0.0).astype(BF), found.astype(BF))
    code[...] = (found * (before + 1.0)).astype(BF)

    pl.semaphore_wait(bar, PLANE - 1 + 3)
    for d in (1, 2, 3):
        pl.semaphore_signal(zsem, inc=1, device_id=dev(rem(z + d, 4), s), device_id_type=MESH)

    def build(gi, carry):
        r = lax.broadcasted_iota(jnp.int32, (256, 128), 0) + gi * 256
        lane = lax.broadcasted_iota(jnp.int32, (256, 128), 1)
        k = ((r >> 3) * MULT) & (DEV - 1)
        e = ((z + (k >> 5)) & 3) * 32 + ((x + (k >> 3)) & 3) * 8 + ((y + (k >> 1)) & 3) * 2 + ((c + k) & 1)
        pick = jnp.where(e == lane, 1.0, 0.0).astype(BF)
        rep = dot_nt(pick, code[...])
        want = ((r & 3) + 1).astype(F32)
        hit = jnp.where(rep == want, 1.0, 0.0)
        half = (r >> 2) & 1
        row0 = pl.multiple_of(gi * 256, 256)
        p8[pl.ds(row0, 256), 0:128] = jnp.where(half == 0, hit, 0.0).astype(BF)
        p8[pl.ds(row0, 256), 128:256] = jnp.where(half == 1, hit, 0.0).astype(BF)
        return carry

    lax.fori_loop(0, 4, build, 0, unroll=True)

    def fold(o):
        o = o.reshape(32, 8, 1024)
        return jnp.concatenate([o[:, :, 0:512], o[:, :, 512:1024]], axis=1).astype(BF)

    def fill(kind):
        def one(gi, carry):
            row0 = pl.multiple_of(gi * 256, 256)
            send[kind, pl.ds(gi * 32, 32)] = fold(dot(p8[pl.ds(row0, 256), :], xin[kind]))
            return carry

        lax.fori_loop(0, 4, one, 0)

    def push(kind):
        def one(i, carry):
            pltpu.make_async_remote_copy(
                send.at[kind, i], recv.at[kind, i], fsem.at[kind], frsem.at[kind, div(i, 32)],
                device_id=out_to(i), device_id_type=MESH,
            ).start()
            return carry

        lax.fori_loop(1, DEV, one, 0)
        recv[kind, 0] = send[kind, 0]

    load[2].wait()
    xin[0, 0:TOK, :] = cot[:, 0:1024]
    xin[0, TOK:, :] = cot[:, 1024:]
    fill(0)
    pl.semaphore_wait(zsem, 3)
    push(0)

    load[1].wait()
    load[3].wait()
    wide = stream[...].astype(F32)
    inv = lax.rsqrt(jnp.mean(wide * wide, axis=1, keepdims=True) + EPS)
    nrm = wide * inv
    normed[...] = nrm
    xin[1, 0:TOK, :] = (nrm * gain[...])[:, 0:1024].astype(BF)
    xin[1, TOK:, :] = (nrm * gain[...])[:, 1024:].astype(BF)
    fill(1)
    push(1)

    for n in (4, 5, 6, 7):
        load[n].wait()
    tril = lax.broadcasted_iota(jnp.int32, (TOK, TOK), 0) >= lax.broadcasted_iota(jnp.int32, (TOK, TOK), 1)

    def head(h):
        return pl.ds(pl.multiple_of(h * HEAD, HEAD), HEAD)

    def local_kv(h, carry):
        kh = kv[:, head(h)]
        skv[pl.ds(2 * h, 2)] = dot_tn(kh, vv[:, head(h)]).reshape(2, 64, HEAD).astype(BF)
        qt[head(h), :] = qv[:, head(h)].T
        mixb[h] = jnp.where(tril, dot_nt(qv[:, head(h)], kh), 0.0).astype(BF)
        return carry

    lax.fori_loop(0, HEADS, local_kv, 0, unroll=4)

    chip = x * 4 + y
    mine = pl.ds(c * CHIPS, CHIPS)
    theirs = pl.ds((1 - c) * CHIPS, CHIPS)

    def swap(src, dst, part, n):
        cp = pltpu.make_async_remote_copy(
            src.at[part], dst.at[part], wsem.at[n], wrsem.at[n], device_id=dev(z, s + 1 - 2 * c), device_id_type=MESH
        )
        cp.start()
        return cp

    def landed(dst, part, n):
        span = dst.at[part]
        pltpu.make_async_copy(span, span, wrsem.at[n]).wait()

    def scatter(src, dst, base, at, n):
        def one(j, carry):
            k = rem(j * CHIP_MULT, CHIPS)
            x2, y2 = rem(x + div(k, 4), 4), rem(y + rem(k, 4), 4)
            pltpu.make_async_remote_copy(
                src.at[x2 * 4 + y2], dst.at[base + at], asem.at[n], arsem.at[n],
                device_id=dev(z, x2 * 8 + y2 * 2 + c), device_id_type=MESH,
            ).start()
            return carry

        lax.fori_loop(1, CHIPS, one, 0)
        dst[base + at] = src[at]

    reach = sorted(
        [(dx, dy) for dx in range(4) for dy in range(4) if dx + dy],
        key=lambda o: (-min(o[0], 4 - o[0]) - min(o[1], 4 - o[1]), o[0] + 2 * o[1]),
    )

    def scatter_far(src, dst, base, at, n):
        for dx, dy in reach:
            x2, y2 = rem(x + dx, 4), rem(y + dy, 4)
            pltpu.make_async_remote_copy(
                src.at[x2 * 4 + y2], dst.at[base + at], asem.at[n], arsem.at[n],
                device_id=dev(z, x2 * 8 + y2 * 2 + c), device_id_type=MESH,
            ).start()
        dst[base + at] = src[at]

    def arrived(dst, sem):
        span = dst.at[pl.ds(0, CHIPS - 1)]
        pltpu.make_async_copy(span, span, sem).wait()

    swaps = [swap(skv, okv, theirs, 0), swap(skv, okv, mine, 1)]

    own_row = index[pl.ds(here, 1), :]
    own_col = jnp.broadcast_to(own_row.astype(F32), (8, CAP)).T[:, 0:1].astype(jnp.int32)
    wide_row = jnp.broadcast_to(own_row, (CAP, CAP))
    wide_col = jnp.broadcast_to(own_col, (CAP, CAP))
    mate = (wide_row >> 7) == (wide_col >> 7)
    slot_col = jnp.sum(jnp.where(mate & (wide_row < wide_col), 1.0, 0.0), axis=1, keepdims=True)
    slot_row = jnp.sum(jnp.where(mate & (wide_col < wide_row), 1.0, 0.0), axis=0, keepdims=True)

    def place(own, slot):
        src = own >> 7
        k = (
            ((z - (src >> 5)) & 3) * 32 + ((x - (src >> 3)) & 3) * 8 + ((y - (src >> 1)) & 3) * 2 + ((c - src) & 1)
        )
        return ((k * MULT_INV) & (DEV - 1)) * 8 + slot.astype(jnp.int32)

    at_col = place(own_col, slot_col)
    at_row = place(own_row, slot_row)
    tcol = jnp.concatenate([at_col, at_col + 4], axis=0)
    trow = jnp.concatenate([at_row, at_row + 4], axis=1)
    gate_col = jnp.broadcast_to(gates[...], (8, CAP)).T[:, 0:1]

    for n in (8, 9, 10):
        load[n].wait()

    def turn_weights(n, carry):
        c0 = pl.multiple_of(n * 256, 256)
        wgt[:, pl.ds(c0, 256)] = wg[pl.ds(c0, 256), :].T
        wut[:, pl.ds(c0, 256)] = wu[pl.ds(c0, 256), :].T
        wdt[pl.ds(c0, 256), :] = wd[:, pl.ds(c0, 256)].T
        return carry

    lax.fori_loop(0, 8, turn_weights, 0)
    for n in range(4):
        p8t[:, n * 256:(n + 1) * 256] = p8[n * 256:(n + 1) * 256, :].T
    landed(okv, mine, 0)
    tkv[...] = (skv[mine].astype(F32) + okv[mine].astype(F32)).astype(BF)
    scatter(tkv, kv1, 0, chip, 0)

    def settle(kind, dst):
        for gi in range(4):
            first = 1 if gi == 0 else 0
            span = recv.at[kind, pl.ds(gi * 32 + first, 32 - first)]
            pltpu.make_async_copy(span, span, frsem.at[kind, gi]).wait()
            lane = lax.broadcasted_iota(jnp.int32, (512, 256), 1) + gi * 256
            put = jnp.where(lane == tcol, 1.0, 0.0).astype(BF)
            for half in range(2):
                f = recv[kind, pl.ds(gi * 32, 32)].astype(F32).reshape(32, 2, 8, 512)[:, half]
                part = dot(put, f.reshape(256, 512).astype(BF))
                at = slice(half * 512, (half + 1) * 512)
                if gi == 0:
                    acc[:, at] = part
                elif gi < 3:
                    acc[:, at] += part
                else:
                    part = (acc[:, at] + part).astype(BF)
                    dst[:, half * 512:(half + 1) * 512] = part[0:CAP]
                    dst[:, 1024 + half * 512:1024 + (half + 1) * 512] = part[CAP:]

    settle(0, dy)
    gout[...] = (gate_col * dy[...].astype(F32)).astype(BF)
    ghid[...] = dot(gout[...], wdt[...])
    settle(1, rows)

    def front(n, carry):
        c0 = pl.multiple_of(n * 256, 256)
        gp = dot(rows[...], wg[:, pl.ds(c0, 256)])
        up = dot(rows[...], wu[:, pl.ds(c0, 256)])
        gh = ghid[:, pl.ds(c0, 256)]
        sg = jax.nn.sigmoid(gp)
        silu = gp * sg
        hid[:, pl.ds(c0, 256)] = (silu * up).astype(BF)
        dpre[:, pl.ds(c0, 256)] = (gh * up * (sg * (1.0 + gp * (1.0 - sg)))).astype(BF)
        dpre[:, pl.ds(pl.multiple_of(c0 + FF, 256), 256)] = (gh * silu).astype(BF)
        return carry

    lax.fori_loop(0, 3, front, 0, unroll=True)

    def back(n, carry):
        r0 = pl.multiple_of(n * 256, 256)
        gr = dot(dpre[:, 0:FF], wgt[:, pl.ds(r0, 256)]) + dot(dpre[:, FF:], wut[:, pl.ds(r0, 256)])
        h0 = pl.multiple_of(div(n, 4) * 256, 256)
        c0 = pl.multiple_of(rem(n, 4) * 256, 256)
        stacked[pl.ds(h0, 256), pl.ds(c0, 256)] = gr.astype(BF)
        return carry

    lax.fori_loop(0, 8, back, 0, unroll=4)

    def refill(gi, carry):
        r = lax.broadcasted_iota(jnp.int32, (256, 512), 0) + gi * 256
        put = jnp.where(r == trow, 1.0, 0.0).astype(BF)
        rsend[pl.ds(gi * 32, 32)] = fold(dot(put, stacked[...]))
        return carry

    def ret(i, carry):
        pltpu.make_async_remote_copy(
            rsend.at[i], rrecv.at[i], bsem, brsem.at[div(i, 32)], device_id=back_to(i), device_id_type=MESH
        ).start()
        return carry

    lax.fori_loop(0, 2, refill, 0)
    lax.fori_loop(1, 32, ret, 0)
    lax.fori_loop(2, 3, refill, 0)
    lax.fori_loop(32, 64, ret, 0)
    lax.fori_loop(3, 4, refill, 0)
    lax.fori_loop(64, 128, ret, 0)
    rrecv[0] = rsend[0]

    def turn(n, carry):
        c0 = pl.multiple_of(n * 256, 256)
        rowst[pl.ds(c0, 256), :] = rows[:, pl.ds(c0, 256)].T
        return carry

    lax.fori_loop(0, 8, turn, 0)
    for n in range(3):
        hidt[n * 256:(n + 1) * 256, :] = hid[:, n * 256:(n + 1) * 256].T
    outs = [(rowst, rows_o), (gout, gout_o), (hidt, hid_o), (dpre, dpre_o)]
    store = [pltpu.make_async_copy(a, b, osem.at[n]) for n, (a, b) in enumerate(outs)]
    for cp in store:
        cp.start()

    def route(n, total):
        c0 = pl.multiple_of(n * 256, 256)
        eo = dot(hid[...], wd[:, pl.ds(c0, 256)])
        return total + jnp.sum(dy[:, pl.ds(c0, 256)].astype(F32) * eo, axis=1, keepdims=True)

    router_col = lax.fori_loop(0, 8, route, jnp.zeros((CAP, 1), F32))
    router[...] = jnp.broadcast_to(router_col, (CAP, 128)).T[0:1, :]

    arrived(kv1, arsem.at[0])

    def prefix(r, total):
        kvs[r] = total.astype(BF)
        return total + kv1[r].astype(F32)

    lax.fori_loop(0, CHIPS, prefix, jnp.zeros((64, HEAD), F32), unroll=True)
    scatter(kvs, kv2, c * CHIPS, chip, 1)

    for gi in range(4):
        first = 1 if gi == 0 else 0
        span = rrecv.at[pl.ds(gi * 32 + first, 32 - first)]
        pltpu.make_async_copy(span, span, brsem.at[gi]).wait()
        for half in range(2):
            f = rrecv[pl.ds(gi * 32, 32)].astype(F32).reshape(32, 2, 8, 512)[:, half]
            f = f.reshape(256, 512).astype(BF)
            part = dot(p8t[:, gi * 256:(gi + 1) * 256], f)
            for hh in range(2):
                c0 = hh * 1024 + half * 512
                piece = part[hh * TOK:(hh + 1) * TOK, :]
                if gi == 0:
                    gin[:, c0:c0 + 512] = piece
                else:
                    gin[:, c0:c0 + 512] += piece

    gi_ = gin[...]
    nrm = normed[...]

    def spread(stage):
        if stage == 0:
            to = [dev(z, s + 1 - 2 * c)]
        elif stage == 1:
            to = [dev(z, x * 8 + rem(y + d, 4) * 2 + c) for d in (1, 2, 3)]
        elif stage == 2:
            to = [dev(z, rem(x + d, 4) * 8 + y * 2 + c) for d in (1, 2, 3)]
        else:
            to = [dev(rem(z + d, 4), s) for d in (1, 2, 3)]
        cps = [
            pltpu.make_async_remote_copy(
                gpart.at[stage], gland.at[stage, d], gsem.at[stage, d], grsem.at[stage, d],
                device_id=t, device_id_type=MESH,
            )
            for d, t in enumerate(to)
        ]
        for cp in cps:
            cp.start()
        return cps

    def collect(stage, cps):
        for cp in cps:
            cp.wait()
        total = gpart[stage]
        for d in range(len(cps)):
            total = total + gland[stage, d]
        return total

    gpart[0] = jnp.sum(gi_ * nrm, axis=0, keepdims=True)
    cps0 = spread(0)

    gn = gi_ * gain[...]
    wide_g = cot[...].astype(F32) + inv * (gn - nrm * jnp.mean(gn * nrm, axis=1, keepdims=True))
    g[...] = wide_g.astype(BF)
    gcp = pltpu.make_async_copy(g, g_o, osem.at[4])
    gcp.start()
    for part in range(2):
        for n in range(8):
            h = part * 8 + n + (8 - 16 * part) * (1 - c)
            sqg[pl.ds(2 * h, 2)] = dot(qt[head(h), :], g[:, head(h)]).reshape(2, 64, HEAD).astype(BF)
        swaps.append(swap(sqg, oqg, (theirs, mine)[part], 2 + part))
    landed(oqg, mine, 2)
    tqg[...] = (sqg[mine].astype(F32) + oqg[mine].astype(F32)).astype(BF)
    scatter_far(tqg, qg1, 0, chip, 2)
    arrived(kv2, arsem.at[1])
    swaps.append(swap(kv2, kv2, mine, 4))
    gpart[1] = collect(0, cps0)
    cps1 = spread(1)

    def local_terms(h, carry):
        gh = g[:, head(h)]
        mix_a = jnp.where(tril, dot_nt(gh, vv[:, head(h)]), 0.0).astype(BF)
        gin[:, head(h)] = dot(mix_a, kv[:, head(h)])
        pk[:, head(h)] = dot_tn(mix_a, qv[:, head(h)])
        pv[:, head(h)] = dot_tn(mixb[h], gh)
        return carry

    lax.fori_loop(0, HEADS, local_terms, 0, unroll=4)
    arrived(qg1, arsem.at[2])

    def suffix(n, total):
        r = CHIPS - 1 - n
        qgs[r] = total.astype(BF)
        return total + qg1[r].astype(F32)

    lax.fori_loop(0, CHIPS, suffix, jnp.zeros((64, HEAD), F32), unroll=True)
    scatter_far(qgs, qg2, c * CHIPS, chip, 3)
    gpart[2] = collect(1, cps1)
    cps2 = spread(2)
    landed(okv, theirs, 1)
    landed(kv2, theirs, 4)
    second = c.astype(F32)

    def early_terms(h, carry):
        two = pl.ds(2 * h, 2)
        prior = (kv2[two].astype(F32) + second * okv[two].astype(F32)).reshape(HEAD, HEAD).astype(BF)
        gq[:, head(h)] = (scale * (gin[:, head(h)] + dot_nt(g[:, head(h)], prior))).astype(BF)
        return carry

    lax.fori_loop(0, HEADS, early_terms, 0, unroll=4)
    late = [pltpu.make_async_copy(gq, gq_o, osem.at[5])]
    late[0].start()
    gpart[3] = collect(2, cps2)
    cps3 = spread(3)
    arrived(qg2, arsem.at[3])
    swaps.append(swap(qg2, qg2, mine, 5))
    landed(oqg, theirs, 3)
    first = 1.0 - second
    for n in range(HEADS):
        if n == HEADS // 2:
            landed(qg2, theirs, 5)
        h = n + (1 - 2 * (n // 8)) * 8 * c
        at, two = head(h), pl.ds(2 * h, 2)
        later = (qg2[two].astype(F32) + first * oqg[two].astype(F32)).reshape(HEAD, HEAD).astype(BF)
        gk[:, at] = (scale * (pk[:, at] + dot_nt(vv[:, at], later))).astype(BF)
        gv[:, at] = (scale * (pv[:, at] + dot(kv[:, at], later))).astype(BF)
    gpart[4] = collect(3, cps3)
    for n, (a, b) in enumerate([(gk, gk_o), (gv, gv_o), (gpart.at[4], gain_o), (router, router_o)]):
        late.append(pltpu.make_async_copy(a, b, osem.at[6 + n]))
        late[-1].start()

    for kind in (0, 1):
        span = send.at[kind, pl.ds(1, DEV - 1)]
        pltpu.make_async_copy(span, span, fsem.at[kind]).wait()
    span = rsend.at[pl.ds(1, DEV - 1)]
    pltpu.make_async_copy(span, span, bsem).wait()
    for n, buf in enumerate((tkv, kvs, tqg, qgs)):
        arrived(buf, asem.at[n])
    for cp in swaps:
        cp.wait_send()
    for cp in store + [gcp] + late:
        cp.wait()


def call_mega(scale, operands):
    def vm(shape, dtype):
        return pltpu.VMEM(shape, dtype)

    state = (PLANE, 64, HEAD)
    results = [
        ((D, CAP), BF), ((CAP, D), BF), ((FF, CAP), BF), ((CAP, 2 * FF), BF), ((1, CAP), F32),
        ((TOK, D), BF), ((TOK, D), BF), ((TOK, D), BF), ((TOK, D), BF), ((1, D), F32),
    ]
    scratch = [
        vm((TOK, D), BF), vm((TOK, D), BF), vm((1, D), F32), vm((DEV, CAP), jnp.int32), vm((1, CAP), F32),
        vm((D, FF), BF), vm((D, FF), BF), vm((FF, D), BF),
        vm((TOK, D), BF), vm((TOK, D), BF), vm((TOK, D), BF),
        vm((TOK, D), F32), vm((2, 256, 1024), BF), vm((CAP, DEV), F32), vm((TOK, DEV), BF), vm((1024, 256), BF), vm((256, 1024), BF),
        vm((2, DEV, 16, 512), BF), vm((2, DEV, 16, 512), BF), vm((512, 1024), F32), vm((CAP, D), BF),
        vm((CAP, D), BF), vm((CAP, D), BF), vm((CAP, FF), F32), vm((CAP, FF), BF), vm((CAP, 2 * FF), BF),
        vm((D, CAP), BF), vm((FF, CAP), BF), vm((512, 1024), BF),
        vm((FF, D), BF), vm((FF, D), BF), vm((D, FF), BF),
        vm((DEV, 16, 512), BF), vm((DEV, 16, 512), BF),
        vm((TOK, D), F32), vm((TOK, D), BF),
        vm((D, TOK), BF),
    ] + [vm(state, BF)] * 6 + [vm((CHIPS, 64, HEAD), BF)] * 6 + [
        vm((HEADS, HEAD, HEAD), BF), vm((TOK, D), F32), vm((TOK, D), F32),
        vm((TOK, D), BF), vm((TOK, D), BF), vm((TOK, D), BF),
        vm((5, 1, D), F32), vm((4, 3, 1, D), F32), vm((1, CAP), F32),
    ]
    dma = pltpu.SemaphoreType.DMA
    sems = [
        dma((11,)), dma((10,)), dma((2,)), dma((2, 4)), dma, dma((4,)), dma((4,)), dma((4,)), dma((6,)), dma((6,)), dma((4, 3)), dma((4, 3)),
        pltpu.SemaphoreType.REGULAR,
    ]
    return pl.pallas_call(
        functools.partial(mega, scale),
        out_shape=[jax.ShapeDtypeStruct(a, b) for a, b in results],
        in_specs=[pl.BlockSpec(memory_space=pl.ANY)] * 11,
        out_specs=[pl.BlockSpec(memory_space=pl.ANY)] * len(results),
        scratch_shapes=scratch + sems,
        compiler_params=pltpu.CompilerParams(
            collective_id=0, has_side_effects=True, vmem_limit_bytes=63 * 1024 * 1024
        ),
        name="mega",
    )(*operands)


def finish(
    rowst_h, gout_h, hidt_h, dpre_h, router_h, g_h, gq_h, gk_h, gv_h, gain_h,
    gate_o, up_o, down_o, router_o, g_o, gq_o, gk_o, gv_o, gain_o,
    rowst, gout, hidt, dpre, router, g, gq, gk, gv, gain, gate, up, down, lsem, psem, wsem,
):
    ins = [(hidt_h, hidt), (gout_h, gout), (rowst_h, rowst), (dpre_h, dpre)]
    loads = [pltpu.make_async_copy(a, b, lsem.at[n]) for n, (a, b) in enumerate(ins)]
    through = [(g_h, g, g_o), (gq_h, gq, gq_o), (gk_h, gk, gk_o), (gv_h, gv, gv_o), (router_h, router, router_o),
               (gain_h, gain, gain_o)]
    take = [pltpu.make_async_copy(a, b, lsem.at[4 + n]) for n, (a, b, o) in enumerate(through)]
    give = [pltpu.make_async_copy(b, o, psem.at[n]) for n, (a, b, o) in enumerate(through)]
    for cp in loads + take:
        cp.start()
    writes = []

    def put(src, dst, rows):
        cp = pltpu.make_async_copy(src.at[rows], dst.at[rows], wsem.at[len(writes)])
        cp.start()
        writes.append(cp)

    loads[0].wait()
    loads[1].wait()
    for n in range(3):
        r = pl.ds(n * 256, 256)
        for m in range(2):
            col = pl.ds(m * 1024, 1024)
            down[r, col] = dot(hidt[r, :], gout[:, col]).astype(BF)
        put(down, down_o, r)
    loads[2].wait()
    loads[3].wait()
    for n in range(8):
        r = pl.ds(n * 256, 256)
        gate[r, :] = dot(rowst[r, :], dpre[:, 0:FF]).astype(BF)
        put(gate, gate_o, r)
        up[r, :] = dot(rowst[r, :], dpre[:, FF:]).astype(BF)
        put(up, up_o, r)
        if n < len(through):
            take[n].wait()
            give[n].start()
    for cp in give + writes:
        cp.wait()


def call_finish(operands):
    def vm(shape, dtype):
        return pltpu.VMEM(shape, dtype)

    small = [((1, CAP), F32), ((TOK, D), BF), ((TOK, D), BF), ((TOK, D), BF), ((TOK, D), BF), ((1, D), F32)]
    weights = [((D, FF), BF), ((D, FF), BF), ((FF, D), BF)]
    dma = pltpu.SemaphoreType.DMA
    return pl.pallas_call(
        finish,
        out_shape=[jax.ShapeDtypeStruct(a, b) for a, b in weights + small],
        in_specs=[pl.BlockSpec(memory_space=pl.ANY)] * 10,
        out_specs=[pl.BlockSpec(memory_space=pl.ANY)] * 9,
        scratch_shapes=[vm((D, CAP), BF), vm((CAP, D), BF), vm((FF, CAP), BF), vm((CAP, 2 * FF), BF)]
        + [vm(a, b) for a, b in small + weights]
        + [dma((10,)), dma((6,)), dma((19,))],
        compiler_params=pltpu.CompilerParams(vmem_limit_bytes=63 * 1024 * 1024),
        name="finish",
    )(*operands)


def body(stream, cotangent, norm_gain, queries, key_vectors, value_vectors, expert_index, router_gates,
         gate_proj, up_proj, down_proj):
    scale = 1.0 / math.sqrt(HEAD * TOK * PLANE)
    results = call_mega(scale, (
        stream, cotangent, norm_gain[None, :], expert_index, router_gates, gate_proj[0], up_proj[0], down_proj[0],
        queries, key_vectors, value_vectors,
    ))
    gate, up, down, router, g, gq, gk, gv, gain = call_finish(results)
    return (g, gq, gk, gv, gate[None], up[None], down[None], router, gain[0])


def solution(mesh):
    both = ("grp", "seq")
    r2, r3 = P(both, None), P(both, None, None)
    return jax.shard_map(
        body,
        mesh=mesh,
        in_specs=(r2, r2, P(), r2, r2, r2, P(), r2, r3, r3, r3),
        out_specs=(r2, r2, r2, r2, r3, r3, r3, r2, P()),
        check_vma=False,
    )
```
